32 devices in a mesh: dp: 8 (over y, x, core), tp: 4 (over z).
Axes of the slice: x: 2, y: 2, z: 4, core: 2. Of those that a mesh axis runs over, the one named last changes fastest.
Arguments:
- slope_up: float32 [8, 1280, 5120], P('dp', None, 'tp'), may hold values from -0.875 to 0.875
- slope_down: float32 [8, 5120, 1280], P('dp', 'tp'), may hold values from -0.875 to 0.875
- slope_norm: float32 [8, 1280], P('dp'), may hold values from -8 to 8
- slope_bias: float32 [8, 1280], P('dp'), may hold values from -8 to 8
- param_up: float32 [1280, 5120], P('dp', 'tp'), may hold values from -0.15625 to 0.15625
- param_down: float32 [5120, 1280], P('tp', 'dp'), may hold values from -0.078125 to 0.078125
- param_norm: float32 [1280], P('dp'), may hold values from 0.25 to 1.75
- param_bias: float32 [1280], P('dp'), may hold values from -3 to 3
- state_up: float32 [1280, 5120], P('dp', 'tp'), may hold values from -1.75 to 1.75
- state_down: float32 [5120, 1280], P('tp', 'dp'), may hold values from -1.75 to 1.75
- state_norm: float32 [1280], P('dp'), may hold values from -1.75 to 1.75
- state_bias: float32 [1280], P('dp'), may hold values from -1.75 to 1.75
Outputs:
- half_up: bfloat16 [1280, 5120], P(None, 'tp')
- half_down: bfloat16 [5120, 1280], P('tp')
- half_norm: bfloat16 [1280], replicated
- half_bias: bfloat16 [1280], replicated
- next_up: float32 [1280, 5120], P('dp', 'tp')
- next_down: float32 [5120, 1280], P('tp', 'dp')
- next_norm: float32 [1280], P('dp')
- next_bias: float32 [1280], P('dp')
- state_new_up: float32 [1280, 5120], P('dp', 'tp')
- state_new_down: float32 [5120, 1280], P('tp', 'dp')
- state_new_norm: float32 [1280], P('dp')
- state_new_bias: float32 [1280], P('dp')
The draws below stay inside these ranges and needn't reach their ends.
All inputs are finite; a program needn't handle non-finite values.
Results may differ from the reference program's by a relative error of at most 0.009.
Values may be sent and summed in bfloat16 or wider, within the bound.
A program may use at most 64 MiB of HBM per device.

```python
import jax
import jax.numpy as jnp

WIDTH = 1280
INNER = 5120
REPLICAS = 8


def strengthened(values, rng, source, target, parts, factor):
    owner, partner = [(jnp.arange(values.shape[position]) // (values.shape[position] // parts)).reshape([-1 if axis == position else 1 for axis in range(values.ndim)]) for position in (source, target)]
    chosen = jax.random.permutation(rng, parts)[partner]
    strong = (owner == chosen) | (owner == (partner + parts // 2) % parts)
    return jnp.where(strong, factor * values, values)


def shard_levels(stream_key, shape, cuts, low, high):
    def one(dim, parts):
        heights = jax.random.uniform(jax.random.fold_in(jax.random.fold_in(stream_key, 6), dim), (parts,), jnp.float32, low / len(cuts), high / len(cuts))
        return jnp.repeat(jnp.exp(heights), shape[dim] // parts).reshape((-1,) + (1,) * (len(shape) - dim - 1))

    factor_of = one(*cuts[0])
    for cut in cuts[1:]:
        factor_of = factor_of * one(*cut)
    return factor_of


def normal_values(key, shape, deviation, bound, pieces=(), dtype=jnp.bfloat16):
    factor_of = shard_levels(key, shape, pieces, -0.22, 0.18) if pieces else 1.0
    array = jax.random.normal(key, shape, jnp.float32) * deviation * factor_of
    return jnp.minimum(jnp.maximum(array, -bound), bound).astype(dtype)


def bell_draw_with(stream_key, extent, spread, reach, split, heavy, kind=jnp.bfloat16):
    result = spread * jax.random.normal(stream_key, extent, jnp.float32)
    if split:
        result = result * shard_levels(stream_key, extent, split, -0.22, 0.18)
    return jnp.clip(strengthened(result, jax.random.fold_in(stream_key, 3), *heavy), -reach, reach).astype(kind)


def setup_inputs(seed: int = 0) -> dict:
    keys = jax.random.split(jax.random.key(seed), 13)
    slope_up = bell_draw_with(keys[0], (REPLICAS, WIDTH, INNER), 0.1, 0.875, ((0, 8), (2, 4)), (0, 1, 8, 2.0), jnp.float32)
    slope_down = bell_draw_with(keys[1], (REPLICAS, INNER, WIDTH), 0.1, 0.875, ((0, 8), (1, 4)), (0, 2, 8, 2.0), jnp.float32)
    slope_norm = bell_draw_with(keys[2], (REPLICAS, WIDTH), 1.0, 8.0, ((0, 8),), (0, 1, 8, 2.0), jnp.float32)
    slope_bias = bell_draw_with(keys[3], (REPLICAS, WIDTH), 1.0, 8.0, ((0, 8),), (0, 1, 8, 2.0), jnp.float32)
    param_up = normal_values(keys[4], (WIDTH, INNER), WIDTH ** -0.5, 0.15625, ((0, 8), (1, 4)), jnp.float32)
    param_down = normal_values(keys[5], (INNER, WIDTH), INNER ** -0.5, 0.078125, ((0, 4), (1, 8)), jnp.float32)
    param_norm = jnp.clip(1.0 + 0.15 * jax.random.normal(keys[6], (WIDTH,), jnp.float32), 0.25, 1.75)
    param_bias = normal_values(keys[7], (WIDTH,), 0.5, 3.0, ((0, 8),), jnp.float32)
    state_up = normal_values(keys[8], (WIDTH, INNER), 0.3, 1.75, ((0, 8), (1, 4)), jnp.float32)
    state_down = normal_values(keys[9], (INNER, WIDTH), 0.3, 1.75, ((0, 4), (1, 8)), jnp.float32)
    state_norm = normal_values(keys[10], (WIDTH,), 0.3, 1.75, ((0, 8),), jnp.float32)
    state_bias = normal_values(keys[11], (WIDTH,), 0.3, 1.75, ((0, 8),), jnp.float32)
    return dict(slope_up=slope_up, slope_down=slope_down, slope_norm=slope_norm, slope_bias=slope_bias, param_up=param_up, param_down=param_down, param_norm=param_norm, param_bias=param_bias, state_up=state_up, state_down=state_down, state_norm=state_norm, state_bias=state_bias)


learn_rate = 0.1
hold_rate = 0.7


def reference(slope_up, slope_down, slope_norm, slope_bias, param_up, param_down, param_norm, param_bias, state_up, state_down, state_norm, state_bias):
    mean_up = jnp.sum(slope_up.astype(jnp.float32), axis=0) * REPLICAS ** -0.5
    mean_down = jnp.sum(slope_down.astype(jnp.float32), axis=0) * REPLICAS ** -0.5
    mean_norm = jnp.sum(slope_norm.astype(jnp.float32), axis=0) * REPLICAS ** -0.5
    mean_bias = jnp.sum(slope_bias.astype(jnp.float32), axis=0) * REPLICAS ** -0.5
    state_new_up = hold_rate * state_up + mean_up
    next_up = param_up - learn_rate * state_new_up
    state_new_down = hold_rate * state_down + mean_down
    next_down = param_down - learn_rate * state_new_down
    state_new_norm = hold_rate * state_norm + mean_norm
    next_norm = param_norm - learn_rate * state_new_norm
    state_new_bias = hold_rate * state_bias + mean_bias
    next_bias = param_bias - learn_rate * state_new_bias
    half_up = next_up.astype(jnp.bfloat16)
    half_down = next_down.astype(jnp.bfloat16)
    half_norm = next_norm.astype(jnp.bfloat16)
    half_bias = next_bias.astype(jnp.bfloat16)
    return half_up, half_down, half_norm, half_bias, next_up, next_down, next_norm, next_bias, state_new_up, state_new_down, state_new_norm, state_new_bias
```

```python
import functools
import math

import jax
import jax.numpy as jnp
from jax import lax
from jax.experimental import pallas as pl
from jax.experimental.pallas import tpu as pltpu
from jax.sharding import PartitionSpec as P

learn_rate = 0.1
hold_rate = 0.7
LANES = 128
GRANT_EXTRA = 2 * 1024 * 1024
F32 = jnp.float32
BF16 = jnp.bfloat16
D2D, RS1, RS2, AG1, AG2, SH1, SH2 = range(7)


def widths_of(half, small):
    if half < 2:
        return [half]
    if small:
        return [1] + widths_of(half - 1, False)
    return [half - half // 2, half // 2]


def slab_plan(columns):
    half = columns // LANES // 2
    slabs = []
    for m in (0, 1):
        start = 0
        for width in widths_of(half, m == 0):
            for axis in (0, 1):
                slabs.append((m, start, width * LANES, axis))
                start += width * LANES
    return slabs


def spot(k):
    y, x, core = k // 4, (k // 2) % 2, k % 2
    return (x, y, core) if core else (y, x, core)


def row_loop(rows, step, fn):
    def go(i, carry):
        fn(pl.ds(pl.multiple_of(i * step, step), step))
        return carry

    lax.fori_loop(0, rows // step, go, 0)


def kernel(
    replicas, slabs, order,
    su, sd, sn, sb, pu, pd, pn, pb, tu, td, tn, tb,
    gu, hd, par, sta, vg, vown,
    fu, fd, bu, bd, r0, r1, r2, gd, vin, vpar, vsta, vb, vr0, vr1, vr2,
    send_sem, recv_sem, vsend_sem, vrecv_sem, load_sem, par_sem, vec_sem,
):
    chunk, columns = pu.shape
    width = replicas * chunk
    me = lax.axis_index("dp")
    c = lax.rem(me, 2)
    x = lax.rem(me // 2, 2)
    y = me // 4
    mate = me + 1 - 2 * c
    x_peer, y_peer = me + 2 - 4 * x, me + 4 - 8 * y
    slow, fast = y + c * (x - y), x + c * (y - x)
    nbr = (x_peer + c * (y_peer - x_peer), y_peer + c * (x_peer - y_peer))
    rate = replicas ** (-0.5)
    step = 32 if chunk % 32 == 0 else 16
    count = len(slabs)
    b, g = (bu, bd), (gu, gd)
    V = count

    barrier = pltpu.get_barrier_semaphore()
    for peer in (mate,) + nbr:
        pl.semaphore_signal(barrier, inc=1, device_id={"dp": peer}, device_id_type=pl.DeviceIdType.MESH)

    def local(src, dst, sem):
        cp = pltpu.make_async_copy(src, dst, sem)
        cp.start()
        return cp

    loads = []
    for i, (m, lo, w, _) in enumerate(slabs):
        if m == 0:
            loads.append(local(su.at[0, :, pl.ds(lo, w)], fu.at[:, pl.ds(lo, w)], load_sem.at[i]))
        else:
            loads.append(local(sd.at[0, pl.ds(lo, w)], fd.at[pl.ds(lo, w)], load_sem.at[i]))
    for n, (whole, pair) in enumerate(((vin, (sn, sb)), (vpar, (pn, pb)), (vsta, (tn, tb)))):
        for row in (0, 1):
            local(pair[row], whole.at[row], vec_sem.at[n])
    for n, (whole, pair) in enumerate(((par, (pu, pd)), (sta, (tu, td)))):
        for m in (0, 1):
            local(pair[m], whole.at[m], par_sem.at[n])

    def loaded(sem, *wholes):
        for n, whole in enumerate(wholes):
            pltpu.make_async_copy(whole, whole, sem.at[n]).wait()

    def convert(i):
        m, lo, w, _ = slabs[i]
        loads[i].wait()
        if m == 0:
            for k in range(replicas):
                bu[*spot(k), :, lo : lo + w] = fu[k * chunk : (k + 1) * chunk, lo : lo + w].astype(BF16)
        else:
            for block in range(width // LANES):
                first = block * LANES
                turned = fd[lo : lo + w, first : first + LANES].T.astype(BF16)
                done = 0
                while done < LANES:
                    k, off = divmod(first + done, chunk)
                    n = min(LANES - done, chunk - off)
                    bd[*spot(k), off : off + n, lo : lo + w] = turned[done : done + n]
                    done += n

    share_of = {D2D: 0, AG1: 0, RS1: 1, AG2: 1, RS2: 2, SH1: 3, SH2: 3}
    vec_out = {D2D: 0, AG2: 0, SH1: 0, RS1: 1, SH2: 1, RS2: 2, AG1: 2}
    vec_in = {D2D: 0, AG1: 0, RS1: 1, AG2: 4, RS2: 2, SH1: 3, SH2: 3}

    def remote(i, kind, src, dst, target):
        if i == V:
            sems = vsend_sem.at[vec_out[kind]], vrecv_sem.at[vec_in[kind]]
        else:
            sems = send_sem.at[kind], recv_sem.at[share_of[kind], i ^ 1 if kind == AG2 else i]
        return pltpu.make_async_remote_copy(
            src_ref=src, dst_ref=dst, send_sem=sems[0], recv_sem=sems[1],
            device_id={"dp": target}, device_id_type=pl.DeviceIdType.MESH,
        )

    copies = {}

    def copy(i, kind, src, dst, target):
        copies[i, kind] = remote(i, kind, src, dst, target)
        copies[i, kind].start()

    def sent(kind, whole):
        remote(0, kind, whole, whole, mate).wait_send()

    def swap(i):
        m, lo, w, _ = slabs[i]
        cols = pl.ds(lo, w)
        copy(i, D2D, b[m].at[:, :, 1 - c, :, cols], r0.at[m, :, :, :, cols], mate)

    def add_to(dst, src, lo, w):
        cols = slice(lo, lo + w)
        dst[:, cols] = dst[:, cols] + src[:, cols]

    def rs1(i, swap_next=None):
        m, lo, w, axis = slabs[i]
        cols = pl.ds(lo, w)
        copies[i, D2D].wait_recv()
        for far in (1, 0):
            for j in (0, 1):
                at = (j, 1 - fast if far else fast) if axis == 0 else (1 - slow if far else slow, j)
                add_to(b[m].at[*at, c], r0.at[m, *at], lo, w)
            if far:
                src = b[m].at[:, 1 - fast, c, :, cols] if axis == 0 else b[m].at[1 - slow, :, c, :, cols]
                copy(i, RS1, src, r1.at[m, :, :, cols], nbr[axis])
                if swap_next is not None:
                    swap(swap_next)

    def rs2(i):
        m, lo, w, axis = slabs[i]
        cols = pl.ds(lo, w)
        copies[i, RS1].wait_recv()
        j = 1 - slow if axis == 0 else 1 - fast
        far = b[m].at[1 - slow, fast, c] if axis == 0 else b[m].at[slow, 1 - fast, c]
        add_to(far, r1.at[m, j], lo, w)
        copy(i, RS2, far.at[:, cols], r2.at[m, :, cols], nbr[1 - axis])
        add_to(b[m].at[slow, fast, c], r1.at[m, 1 - j], lo, w)

    def update(i):
        m, lo, w, axis = slabs[i]
        cs = slice(lo, lo + w)
        cols = pl.ds(lo, w)
        copies[i, RS2].wait_recv()
        own, out = b[m].at[slow, fast, c], g[m].at[slow, fast, c]

        def go(rows):
            mean = (own[rows, cs].astype(F32) + r2[m, rows, cs].astype(F32)) * rate
            state = hold_rate * sta[m, rows, cs] + mean
            new = par[m, rows, cs] - learn_rate * state
            out[rows, cs] = new.astype(BF16)
            sta[m, rows, cs] = state
            par[m, rows, cs] = new

        row_loop(chunk, step, go)
        copy(i, AG1, out.at[:, cols], out.at[:, cols], nbr[1 - axis])

    def ag2(i):
        m, lo, w, axis = slabs[i]
        cols = pl.ds(lo, w)
        copies[i, AG1].wait_recv()
        part = g[m].at[:, fast, c, :, cols] if axis == 0 else g[m].at[slow, :, c, :, cols]
        copy(i, AG2, part, part, nbr[axis])
        copy(i, SH1, part, part, mate)

    def share(i):
        m, lo, w, axis = slabs[i]
        cols = pl.ds(lo, w)
        copies[i, AG2].wait_recv()
        part = g[m].at[:, 1 - fast, c, :, cols] if axis == 0 else g[m].at[1 - slow, :, c, :, cols]
        copy(i, SH2, part, part, mate)

    def finish(i):
        m, lo, w, axis = slabs[i]
        both = g[m].at[:, :, 1 - c, :, pl.ds(lo, w)]
        remote(i, SH2, both, both, mate).wait_recv()
        if m == 1:
            for block in range(width // LANES):
                first, done, parts = block * LANES, 0, []
                while done < LANES:
                    k, off = divmod(first + done, chunk)
                    n = min(LANES - done, chunk - off)
                    parts.append(gd[*spot(k), off : off + n, lo : lo + w].astype(F32))
                    done += n
                whole = parts[0] if len(parts) == 1 else jnp.concatenate(parts, axis=0)
                hd[lo : lo + w, first : first + LANES] = whole.T.astype(BF16)

    def vec_swap():
        loaded(vec_sem, vin, vpar, vsta)
        for row in (0, 1):
            for k in range(replicas):
                vb[*spot(k), row : row + 1, 0:chunk] = vin[row, :, k * chunk : (k + 1) * chunk]
        copy(V, D2D, vb.at[:, :, 1 - c], vr0, mate)

    def vec_rs1():
        copies[V, D2D].wait_recv()
        for at in ((0, 0), (0, 1), (1, 0), (1, 1)):
            vb[*at, c] = vb[*at, c] + vr0[*at]
        copy(V, RS1, vb.at[:, 1 - fast, c], vr1, nbr[0])

    def vec_rs2():
        copies[V, RS1].wait_recv()
        for j in (0, 1):
            vb[j, fast, c] = vb[j, fast, c] + vr1[j]
        copy(V, RS2, vb.at[1 - slow, fast, c], vr2, nbr[1])

    def vec_update():
        copies[V, RS2].wait_recv()
        mean = (vb[slow, fast, c] + vr2[...]) * rate
        for row in (0, 1):
            state = hold_rate * vsta[row] + mean[row : row + 1, 0:chunk]
            new = vpar[row] - learn_rate * state
            vg[slow, fast, c, row : row + 1, 0:chunk] = new
            vown[row] = new
            vown[2 + row] = state
        copy(V, AG1, vg.at[slow, fast, c], vg.at[slow, fast, c], nbr[1])

    def vec_ag2():
        copies[V, AG1].wait_recv()
        part = vg.at[:, fast, c]
        copy(V, AG2, part, part, nbr[0])
        copy(V, SH1, part, part, mate)

    def vec_share():
        copies[V, AG2].wait_recv()
        part = vg.at[:, 1 - fast, c]
        copy(V, SH2, part, part, mate)

    vb[...] = jnp.zeros_like(vb)
    vg[slow, fast, c] = jnp.zeros(vr2.shape, F32)
    convert(0)
    pl.semaphore_wait(barrier, 3)
    swap(0)
    convert(1)
    swap(1)
    for i in range(2, count):
        convert(i)
        rs1(i - 2, i)
        if i == 6:
            vec_swap()
        if i == 8:
            vec_rs1()
    rs1(count - 2)
    rs1(count - 1)

    for i in range(count):
        rs2(i)
        if i == 4:
            sent(D2D, r0)
            vec_rs2()
    loaded(par_sem, par, sta)
    for n, i in enumerate(list(range(2, count)) + [0, 1]):
        update(i)
        if n == 0:
            vec_update()
            sent(RS1, r1)
    for n, i in enumerate(order):
        ag2(i)
        if n == 0:
            vec_ag2()
            sent(RS2, r2)
    for n, i in enumerate(order):
        share(i)
        if n == 0:
            sent(AG1, r2)
        if n == 1:
            vec_share()
        if n:
            finish(order[n - 1])
    other = vg.at[:, :, 1 - c]
    remote(V, SH2, other, other, mate).wait_recv()
    for whole, kind in ((vb, D2D), (vr0, RS1), (vr1, RS2)):
        remote(V, kind, whole, whole, mate).wait_send()
    sent(SH1, r1)
    sent(AG2, r1)
    finish(order[-1])
    sent(SH2, r1)


def spill(
    replicas, chunk,
    hu, hd, par, sta, vg, vown,
    hu_out, hd_out, nu_out, nd_out, tu_out, td_out, nn_out, nb_out, tn_out, tb_out, hn_out, hb_out,
    hv0, hv1, sem,
):
    width = replicas * chunk
    vw = columns_pad(chunk)
    for k in range(replicas):
        pltpu.make_async_copy(hu.at[*spot(k)], hu_out.at[pl.ds(k * chunk, chunk)], sem.at[0]).start()
    moves = [
        (hd, hd_out), (par.at[0], nu_out), (par.at[1], nd_out), (sta.at[0], tu_out), (sta.at[1], td_out),
        (vown.at[0], nn_out), (vown.at[1], nb_out), (vown.at[2], tn_out), (vown.at[3], tb_out),
        (hv0, hn_out), (hv1, hb_out),
    ]
    stores = [pltpu.make_async_copy(src, dst, sem.at[i + 1]) for i, (src, dst) in enumerate(moves)]
    for cp in stores[:-2]:
        cp.start()
    lane = lax.broadcasted_iota(jnp.int32, (2, width), 1)
    full = jnp.zeros((2, width), F32)
    for k in range(replicas):
        piece = vg[*spot(k)]
        wide = jnp.concatenate([piece, jnp.zeros((2, width - vw), F32)], axis=1) if width > vw else piece
        moved = pltpu.roll(wide, k * chunk, 1) if k else wide
        full = jnp.where((lane >= k * chunk) & (lane < (k + 1) * chunk), moved, full)
    for row, out in enumerate((hv0, hv1)):
        out[...] = full[row].astype(BF16)
    for cp in stores[-2:]:
        cp.start()
    for cp in stores:
        cp.wait()
    pltpu.make_async_copy(hu_out, hu_out, sem.at[0]).wait()


def columns_pad(n):
    return -(-n // LANES) * LANES


def fused(slope_up, slope_down, slope_norm, slope_bias, param_up, param_down, param_norm, param_bias,
          state_up, state_down, state_norm, state_bias):
    replicas = lax.axis_size("dp")
    chunk, columns = param_up.shape
    width = replicas * chunk
    slabs = slab_plan(columns)
    count = len(slabs)
    per = len([s for s in slabs if s[0] == 0])
    order = list(range(2, 4)) + list(range(per, count)) + list(range(4, per)) + [0, 1]
    vw = columns_pad(chunk)
    hbm = pl.BlockSpec(memory_space=pl.ANY)
    vmem = pl.BlockSpec(memory_space=pltpu.VMEM)
    cube = (2, 2, 2, chunk, columns)
    shape = jax.ShapeDtypeStruct
    dma = pltpu.SemaphoreType.DMA
    row = lambda v: v.reshape(1, -1)
    scratch = [
        pltpu.VMEM((width, columns), F32), pltpu.VMEM((columns, width), F32),
        pltpu.VMEM(cube, BF16), pltpu.VMEM(cube, BF16),
        pltpu.VMEM((2, 2, 2, chunk, columns), BF16),
        pltpu.VMEM((2, 2, chunk, columns), BF16),
        pltpu.VMEM((2, chunk, columns), BF16),
        pltpu.VMEM(cube, BF16),
        pltpu.VMEM((2, 1, width), F32), pltpu.VMEM((2, 1, chunk), F32), pltpu.VMEM((2, 1, chunk), F32),
        pltpu.VMEM((2, 2, 2, 2, vw), F32), pltpu.VMEM((2, 2, 2, vw), F32),
        pltpu.VMEM((2, 2, vw), F32), pltpu.VMEM((2, vw), F32),
    ]
    grant = sum(math.prod(s.shape) * jnp.dtype(s.dtype).itemsize for s in scratch) + GRANT_EXTRA
    hu, hd, par, sta, vg, vown = pl.pallas_call(
        functools.partial(kernel, replicas, slabs, order),
        out_shape=(
            pltpu.VMEM(cube, BF16), pltpu.VMEM((columns, width), BF16),
            pltpu.VMEM((2, chunk, columns), F32), pltpu.VMEM((2, chunk, columns), F32),
            pltpu.VMEM((2, 2, 2, 2, vw), F32), pltpu.VMEM((4, 1, chunk), F32),
        ),
        in_specs=[hbm] * 12,
        out_specs=[vmem] * 6,
        scratch_shapes=scratch + [
            dma((SH2 + 1,)), dma((4, count)), dma((3,)), dma((5,)),
            dma((count,)), dma((2,)), dma((3,)),
        ],
        compiler_params=pltpu.CompilerParams(collective_id=0, has_side_effects=True, vmem_limit_bytes=grant),
    )(*(pltpu.with_memory_space_constraint(v, pltpu.HBM) for v in (
        slope_up, slope_down, slope_norm, slope_bias,
        param_up, param_down.T, row(param_norm), row(param_bias),
        state_up, state_down.T, row(state_norm), row(state_bias),
    )))
    block, line = shape((chunk, columns), F32), shape((1, chunk), F32)
    half = shape((width,), BF16)
    hu, hd, nu, nd, tu, td, nn, nb, tn, tb, hn, hb = pl.pallas_call(
        functools.partial(spill, replicas, chunk),
        out_shape=(shape((width, columns), BF16), shape((columns, width), BF16)) + (block,) * 4 + (line,) * 4 + (half,) * 2,
        in_specs=[vmem] * 6,
        out_specs=[hbm] * 12,
        scratch_shapes=[pltpu.VMEM((width,), BF16), pltpu.VMEM((width,), BF16), dma((12,))],
        compiler_params=pltpu.CompilerParams(vmem_limit_bytes=GRANT_EXTRA),
    )(hu, hd, par, sta, vg, vown)
    flat = lambda v: v.reshape(-1)
    return hu, hd, hn, hb, nu, nd.T, flat(nn), flat(nb), tu, td.T, flat(tn), flat(tb)


def plain(slope_up, slope_down, slope_norm, slope_bias, param_up, param_down, param_norm, param_bias,
          state_up, state_down, state_norm, state_bias):
    rate = lax.axis_size("dp") ** (-0.5)
    place = lax.axis_index("dp")

    def step(mean, param, state):
        state_new = hold_rate * state + mean * rate
        return param - learn_rate * state_new, state_new

    def scattered(slope, dim):
        return lax.psum_scatter(slope[0].astype(BF16), "dp", scatter_dimension=dim, tiled=True).astype(F32)

    def gathered(value, dim):
        return lax.all_gather(value.astype(BF16), "dp", axis=dim, tiled=True)

    sums = lax.psum((slope_norm[0], slope_bias[0]), "dp")
    size = param_norm.shape[0]
    own = [lax.dynamic_slice_in_dim(v, place * size, size) for v in sums]
    nu, tu = step(scattered(slope_up, 0), param_up, state_up)
    nd, td = step(scattered(slope_down, 1), param_down, state_down)
    nn, tn = step(own[0], param_norm, state_norm)
    nb, tb = step(own[1], param_bias, state_bias)
    halves = gathered(nu, 0), gathered(nd, 1), gathered(nn, 0), gathered(nb, 0)
    return halves + (nu, nd, nn, nb, tu, td, tn, tb)


def body(*args):
    replicas = lax.axis_size("dp")
    chunk, columns = args[4].shape
    fits = replicas == 2 ** 3 and chunk % 16 == 0 and columns % (2 * LANES) == 0
    fits = fits and (replicas * chunk) % LANES == 0
    return (fused if fits else plain)(*args)


def solution(mesh):
    matrices = (P("dp", "tp"), P("tp", "dp"), P("dp"), P("dp"))
    return jax.shard_map(
        body,
        mesh=mesh,
        in_specs=(P("dp", None, "tp"), P("dp", "tp", None), P("dp", None), P("dp", None)) + matrices * 2,
        out_specs=(P(None, "tp"), P("tp", None), P(), P()) + matrices * 2,
        check_vma=False,
    )
```

```python
import functools
import math

import jax
import jax.numpy as jnp
from jax import lax
from jax.experimental import pallas as pl
from jax.experimental.pallas import tpu as pltpu
from jax.sharding import PartitionSpec as P

learn_rate = 0.1
hold_rate = 0.7
LANES = 128
GRANT_EXTRA = 2 * 1024 * 1024
F32 = jnp.float32
BF16 = jnp.bfloat16
FAR, NEAR, RS1, RS2, AG1, AG2, SH1, SH2, END, OVER = range(10)


def widths_of(half, small):
    if half < 2:
        return [half]
    if small:
        return [1] + widths_of(half - 1, False)
    return [half - half // 2, half // 2]


def slab_plan(columns):
    half = columns // LANES // 2
    slabs = []
    for m in (0, 1):
        start = 0
        for width in widths_of(half, m == 0):
            for axis in (0, 1):
                slabs.append((m, start, width * LANES, axis))
                start += width * LANES
    return slabs


def spot(k):
    y, x, core = k // 4, (k // 2) % 2, k % 2
    return (x, y, core) if core else (y, x, core)


def row_loop(rows, step, fn):
    def go(i, carry):
        fn(pl.ds(pl.multiple_of(i * step, step), step))
        return carry

    lax.fori_loop(0, rows // step, go, 0)


def kernel(
    replicas, slabs, order,
    su, sd, sn, sb, pu, pd, pn, pb, tu, td, tn, tb,
    gu, hd, par, sta, vg, vown,
    fu, fd, bu, bd, r0, r1, r2, gd, vin, vpar, vsta, vb, vr0, vr1, vr2,
    send_sem, recv_sem, vsend_sem, vrecv_sem, load_sem, par_sem, vec_sem,
):
    chunk, columns = pu.shape
    width = replicas * chunk
    me = lax.axis_index("dp")
    c = lax.rem(me, 2)
    x = lax.rem(me // 2, 2)
    y = me // 4
    mate = me + 1 - 2 * c
    x_peer, y_peer = me + 2 - 4 * x, me + 4 - 8 * y
    slow, fast = y + c * (x - y), x + c * (y - x)
    nbr = (x_peer + c * (y_peer - x_peer), y_peer + c * (x_peer - y_peer))
    rate = replicas ** (-0.5)
    step = 32 if chunk % 32 == 0 else 16
    count = len(slabs)
    per = len([s for s in slabs if s[0] == 0])
    b, g = (bu, bd), (gu, gd)
    V = count

    over = tuple(peer + 1 - 2 * c for peer in nbr)
    kept = chunk - chunk * 4 // 10 // 16 * 16

    barrier = pltpu.get_barrier_semaphore()
    for peer in (mate,) + nbr + over:
        pl.semaphore_signal(barrier, inc=1, device_id={"dp": peer}, device_id_type=pl.DeviceIdType.MESH)

    def local(src, dst, sem):
        cp = pltpu.make_async_copy(src, dst, sem)
        cp.start()
        return cp

    loads = {}
    for i, (m, lo, w, axis) in enumerate(slabs):
        if i > 3 and axis == 1:
            continue
        span = pl.ds(lo, w if i < 4 else 2 * w)
        if m == 0:
            loads[i] = local(su.at[0, :, span], fu.at[:, span], load_sem.at[len(loads)])
        else:
            loads[i] = local(sd.at[0, span], fd.at[span], load_sem.at[len(loads)])
    for n, (whole, pair) in enumerate(((vin, (sn, sb)), (vpar, (pn, pb)), (vsta, (tn, tb)))):
        for row in (0, 1):
            local(pair[row], whole.at[row], vec_sem.at[n])
    for n, (whole, pair) in enumerate(((par, (pu, pd)), (sta, (tu, td)))):
        for m in (0, 1):
            local(pair[m], whole.at[m], par_sem.at[n])

    def loaded(sem, *wholes):
        for n, whole in enumerate(wholes):
            pltpu.make_async_copy(whole, whole, sem.at[n]).wait()

    def convert(i):
        m, lo, w, _ = slabs[i]
        if i in loads:
            loads[i].wait()
        if m == 0:
            for k in range(replicas):
                bu[*spot(k), :, lo : lo + w] = fu[k * chunk : (k + 1) * chunk, lo : lo + w].astype(BF16)
        else:
            for block in range(width // LANES):
                first = block * LANES
                turned = fd[lo : lo + w, first : first + LANES].T.astype(BF16)
                done = 0
                while done < LANES:
                    k, off = divmod(first + done, chunk)
                    n = min(LANES - done, chunk - off)
                    bd[*spot(k), off : off + n, lo : lo + w] = turned[done : done + n]
                    done += n

    leave = {FAR: 0, NEAR: 0, AG2: 1, END: 1, SH1: 1, RS1: 2, SH2: 2, OVER: 2, RS2: 3, AG1: 3}
    vec_out = {FAR: 0, AG2: 0, SH1: 0, RS1: 1, SH2: 1, RS2: 2, AG1: 2}
    vec_in = {FAR: 0, AG1: 0, RS1: 1, AG2: 4, RS2: 2, SH1: 3, SH2: 3}

    def arrival(i, kind):
        if kind in (SH1, SH2, OVER):
            return 3 * count + (1 + (i - per) // 2 if slabs[i][0] else 0)
        if kind in (NEAR, END):
            return 3 * count + 1 + (count - per) // 2 + (kind == END)
        return {FAR: 0, AG1: 0, RS1: 1, AG2: 1, RS2: 2}[kind] * count + (i ^ 1 if kind == AG2 else i)

    def remote(i, kind, src, dst, target):
        if i == V:
            sems = vsend_sem.at[vec_out[kind]], vrecv_sem.at[vec_in[kind]]
        else:
            sems = send_sem.at[leave[kind]], recv_sem.at[arrival(i, kind)]
        return pltpu.make_async_remote_copy(
            src_ref=src, dst_ref=dst, send_sem=sems[0], recv_sem=sems[1],
            device_id={"dp": target}, device_id_type=pl.DeviceIdType.MESH,
        )

    copies = {}

    def copy(i, kind, src, dst, target):
        copies[i, kind] = remote(i, kind, src, dst, target)
        copies[i, kind].start()

    def sent(kind, whole):
        remote(0, kind, whole, whole, mate).wait_send()

    def swap(i, kind):
        m, lo, w, axis = slabs[i]
        cols = pl.ds(lo, w)
        if axis == 0:
            at = 1 - slow if kind == FAR else slow
            copy(i, kind, b[m].at[:, at, 1 - c, :, cols], r0.at[m, :, at, :, cols], mate)
        else:
            at = 1 - fast if kind == FAR else fast
            copy(i, kind, b[m].at[at, :, 1 - c, :, cols], r0.at[m, at, :, :, cols], mate)

    def rs1(i):
        m, lo, w, axis = slabs[i]
        cols = pl.ds(lo, w)
        copies[i, FAR].wait_recv()
        for j in (0, 1):
            at = (j, 1 - fast) if axis == 0 else (1 - slow, j)
            b[m][*at, c, :, lo : lo + w] = b[m][*at, c, :, lo : lo + w] + r0[m, *at, :, lo : lo + w]
        src = b[m].at[:, 1 - fast, c, :, cols] if axis == 0 else b[m].at[1 - slow, :, c, :, cols]
        copy(i, RS1, src, r1.at[m, :, :, cols], nbr[axis])

    def rs2(i):
        m, lo, w, axis = slabs[i]
        cs = slice(lo, lo + w)
        cols = pl.ds(lo, w)
        copies[i, RS1].wait_recv()
        j = 1 - slow if axis == 0 else 1 - fast
        far = (1 - slow, fast) if axis == 0 else (slow, 1 - fast)
        b[m][*far, c, :, cs] = b[m][*far, c, :, cs] + r0[m, *far, :, cs] + r1[m, j, :, cs]
        copy(i, RS2, b[m].at[*far, c, :, cols], r2.at[m, :, cols], nbr[1 - axis])
        own = slow, fast
        b[m][*own, c, :, cs] = b[m][*own, c, :, cs] + r0[m, *own, :, cs] + r1[m, 1 - j, :, cs]

    def update(i):
        m, lo, w, axis = slabs[i]
        cs = slice(lo, lo + w)
        cols = pl.ds(lo, w)
        copies[i, RS2].wait_recv()
        own, out = b[m].at[slow, fast, c], g[m].at[slow, fast, c]

        def go(rows):
            mean = (own[rows, cs].astype(F32) + r2[m, rows, cs].astype(F32)) * rate
            state = hold_rate * sta[m, rows, cs] + mean
            new = par[m, rows, cs] - learn_rate * state
            out[rows, cs] = new.astype(BF16)
            sta[m, rows, cs] = state
            par[m, rows, cs] = new

        row_loop(chunk, step, go)
        copy(i, AG1, out.at[:, cols], out.at[:, cols], nbr[1 - axis])

    def ag2(i):
        m, lo, w, axis = slabs[i]
        cols = pl.ds(lo, w)
        copies[i, AG1].wait_recv()
        part = g[m].at[:, fast, c] if axis == 0 else g[m].at[slow, :, c]
        early = part.at[:, pl.ds(0, kept if i < 2 else chunk), cols]
        copy(i, AG2, early, early, nbr[axis])
        copy(i, SH1, part.at[:, :, cols], part.at[:, :, cols], mate)

    def ends():
        for i in (0, 1):
            m, lo, w, axis = slabs[i]
            part = g[m].at[:, fast, c] if axis == 0 else g[m].at[slow, :, c]
            rest = part.at[:, pl.ds(kept, chunk - kept), pl.ds(lo, w)]
            copy(i, END, rest, rest, nbr[axis])
            copy(i, OVER, rest, rest, over[axis])

    def share(i):
        m, lo, w, axis = slabs[i]
        cols = pl.ds(lo, w)
        copies[i, AG2].wait_recv()
        part = g[m].at[:, 1 - fast, c] if axis == 0 else g[m].at[1 - slow, :, c]
        part = part.at[:, pl.ds(0, kept if i < 2 else chunk), cols]
        copy(i, SH2, part, part, mate)

    def finish(i):
        m, lo, w, axis = slabs[i]
        if m == 1:
            if axis == 0:
                pair = gd.at[:, :, 1 - c, :, pl.ds(lo, 2 * w)]
                remote(i, SH2, pair, pair, mate).wait_recv()
            for block in range(width // LANES):
                first, done, parts = block * LANES, 0, []
                while done < LANES:
                    k, off = divmod(first + done, chunk)
                    n = min(LANES - done, chunk - off)
                    parts.append(gd[*spot(k), off : off + n, lo : lo + w].astype(F32))
                    done += n
                whole = parts[0] if len(parts) == 1 else jnp.concatenate(parts, axis=0)
                hd[lo : lo + w, first : first + LANES] = whole.T.astype(BF16)

    def vec_swap():
        loaded(vec_sem, vin, vpar, vsta)
        for row in (0, 1):
            for k in range(replicas):
                vb[*spot(k), row : row + 1, 0:chunk] = vin[row, :, k * chunk : (k + 1) * chunk]
        copy(V, FAR, vb.at[:, :, 1 - c], vr0, mate)

    def vec_rs1():
        copies[V, FAR].wait_recv()
        for at in ((0, 0), (0, 1), (1, 0), (1, 1)):
            vb[*at, c] = vb[*at, c] + vr0[*at]
        copy(V, RS1, vb.at[:, 1 - fast, c], vr1, nbr[0])

    def vec_rs2():
        copies[V, RS1].wait_recv()
        for j in (0, 1):
            vb[j, fast, c] = vb[j, fast, c] + vr1[j]
        copy(V, RS2, vb.at[1 - slow, fast, c], vr2, nbr[1])

    def vec_update():
        copies[V, RS2].wait_recv()
        mean = (vb[slow, fast, c] + vr2[...]) * rate
        for row in (0, 1):
            state = hold_rate * vsta[row] + mean[row : row + 1, 0:chunk]
            new = vpar[row] - learn_rate * state
            vg[slow, fast, c, row : row + 1, 0:chunk] = new
            vown[row] = new
            vown[2 + row] = state
        copy(V, AG1, vg.at[slow, fast, c], vg.at[slow, fast, c], nbr[1])

    def vec_ag2():
        copies[V, AG1].wait_recv()
        part = vg.at[:, fast, c]
        copy(V, AG2, part, part, nbr[0])
        copy(V, SH1, part, part, mate)

    def vec_share():
        copies[V, AG2].wait_recv()
        part = vg.at[:, 1 - fast, c]
        copy(V, SH2, part, part, mate)

    vb[...] = jnp.zeros_like(vb)
    vg[slow, fast, c] = jnp.zeros(vr2.shape, F32)
    convert(0)
    pl.semaphore_wait(barrier, 5)
    swap(0, FAR)
    convert(1)
    swap(1, FAR)
    for i in range(2, count):
        convert(i)
        swap(i, FAR)
        rs1(i - 2)
        if i == 6:
            vec_swap()
        if i == 8:
            vec_rs1()
    for i in (count - 2, count - 1):
        rs1(i)
    for i in range(count):
        swap(i, NEAR)
    remote(0, NEAR, r1, r1, mate).wait_recv()

    for i in range(count):
        rs2(i)
        if i == 4:
            sent(FAR, r0)
        if i == 7:
            vec_rs2()
    loaded(par_sem, par, sta)
    for n, i in enumerate(list(range(2, count)) + [0, 1]):
        update(i)
        if n == 6:
            vec_update()
    for n, i in enumerate(order):
        ag2(i)
        if n == 4:
            vec_ag2()
    ends()
    for n, i in enumerate(order):
        share(i)
        if n == 0:
            sent(RS2, r1)
        if n == 5:
            vec_share()
        if n > 1:
            finish(order[n - 2])
    finish(order[-2])
    finish(order[-1])
    other = vg.at[:, :, 1 - c]
    remote(V, SH2, other, other, mate).wait_recv()
    for whole, kind in ((vb, FAR), (vr0, RS1), (vr1, RS2)):
        remote(V, kind, whole, whole, mate).wait_send()
    rest = gu.at[:, 0, c, pl.ds(kept, chunk - kept), pl.ds(0, 2 * slabs[0][2])]
    remote(0, END, rest, rest, mate).wait_recv()
    whole = gu.at[:, :, 1 - c]
    remote(0, SH2, whole, whole, mate).wait_recv()
    sent(AG2, r0)
    sent(SH2, r0)


def spill(
    replicas, chunk,
    hu, hd, par, sta, vg, vown,
    hu_out, hd_out, nu_out, nd_out, tu_out, td_out, nn_out, nb_out, tn_out, tb_out, hn_out, hb_out,
    hv0, hv1, sem,
):
    width = replicas * chunk
    vw = columns_pad(chunk)
    for k in range(replicas):
        pltpu.make_async_copy(hu.at[*spot(k)], hu_out.at[pl.ds(k * chunk, chunk)], sem.at[0]).start()
    moves = [
        (hd, hd_out), (par.at[0], nu_out), (par.at[1], nd_out), (sta.at[0], tu_out), (sta.at[1], td_out),
        (vown.at[0], nn_out), (vown.at[1], nb_out), (vown.at[2], tn_out), (vown.at[3], tb_out),
        (hv0, hn_out), (hv1, hb_out),
    ]
    stores = [pltpu.make_async_copy(src, dst, sem.at[i + 1]) for i, (src, dst) in enumerate(moves)]
    for cp in stores[:-2]:
        cp.start()
    lane = lax.broadcasted_iota(jnp.int32, (2, width), 1)
    full = jnp.zeros((2, width), F32)
    for k in range(replicas):
        piece = vg[*spot(k)]
        wide = jnp.concatenate([piece, jnp.zeros((2, width - vw), F32)], axis=1) if width > vw else piece
        moved = pltpu.roll(wide, k * chunk, 1) if k else wide
        full = jnp.where((lane >= k * chunk) & (lane < (k + 1) * chunk), moved, full)
    for row, out in enumerate((hv0, hv1)):
        out[...] = full[row].astype(BF16)
    for cp in stores[-2:]:
        cp.start()
    for cp in stores:
        cp.wait()
    pltpu.make_async_copy(hu_out, hu_out, sem.at[0]).wait()


def columns_pad(n):
    return -(-n // LANES) * LANES


def fused(slope_up, slope_down, slope_norm, slope_bias, param_up, param_down, param_norm, param_bias,
          state_up, state_down, state_norm, state_bias):
    replicas = lax.axis_size("dp")
    chunk, columns = param_up.shape
    width = replicas * chunk
    slabs = slab_plan(columns)
    count = len(slabs)
    per = len([s for s in slabs if s[0] == 0])
    order = list(range(2, 4)) + list(range(per, count)) + list(range(4, per)) + [0, 1]
    vw = columns_pad(chunk)
    hbm = pl.BlockSpec(memory_space=pl.ANY)
    vmem = pl.BlockSpec(memory_space=pltpu.VMEM)
    cube = (2, 2, 2, chunk, columns)
    shape = jax.ShapeDtypeStruct
    dma = pltpu.SemaphoreType.DMA
    row = lambda v: v.reshape(1, -1)
    scratch = [
        pltpu.VMEM((width, columns), F32), pltpu.VMEM((columns, width), F32),
        pltpu.VMEM(cube, BF16), pltpu.VMEM(cube, BF16),
        pltpu.VMEM((2, 2, 2, chunk, columns), BF16),
        pltpu.VMEM((2, 2, chunk, columns), BF16),
        pltpu.VMEM((2, chunk, columns), BF16),
        pltpu.VMEM(cube, BF16),
        pltpu.VMEM((2, 1, width), F32), pltpu.VMEM((2, 1, chunk), F32), pltpu.VMEM((2, 1, chunk), F32),
        pltpu.VMEM((2, 2, 2, 2, vw), F32), pltpu.VMEM((2, 2, 2, vw), F32),
        pltpu.VMEM((2, 2, vw), F32), pltpu.VMEM((2, vw), F32),
    ]
    grant = sum(math.prod(s.shape) * jnp.dtype(s.dtype).itemsize for s in scratch) + GRANT_EXTRA
    hu, hd, par, sta, vg, vown = pl.pallas_call(
        functools.partial(kernel, replicas, slabs, order),
        out_shape=(
            pltpu.VMEM(cube, BF16), pltpu.VMEM((columns, width), BF16),
            pltpu.VMEM((2, chunk, columns), F32), pltpu.VMEM((2, chunk, columns), F32),
            pltpu.VMEM((2, 2, 2, 2, vw), F32), pltpu.VMEM((4, 1, chunk), F32),
        ),
        in_specs=[hbm] * 12,
        out_specs=[vmem] * 6,
        scratch_shapes=scratch + [
            dma((4,)), dma((3 * count + 3 + (count - per) // 2,)), dma((3,)), dma((5,)),
            dma((2 + count // 2,)), dma((2,)), dma((3,)),
        ],
        compiler_params=pltpu.CompilerParams(collective_id=0, has_side_effects=True, vmem_limit_bytes=grant),
    )(*(pltpu.with_memory_space_constraint(v, pltpu.HBM) for v in (
        slope_up, slope_down, slope_norm, slope_bias,
        param_up, param_down.T, row(param_norm), row(param_bias),
        state_up, state_down.T, row(state_norm), row(state_bias),
    )))
    block, line = shape((chunk, columns), F32), shape((1, chunk), F32)
    half = shape((width,), BF16)
    hu, hd, nu, nd, tu, td, nn, nb, tn, tb, hn, hb = pl.pallas_call(
        functools.partial(spill, replicas, chunk),
        out_shape=(shape((width, columns), BF16), shape((columns, width), BF16)) + (block,) * 4 + (line,) * 4 + (half,) * 2,
        in_specs=[vmem] * 6,
        out_specs=[hbm] * 12,
        scratch_shapes=[pltpu.VMEM((width,), BF16), pltpu.VMEM((width,), BF16), dma((12,))],
        compiler_params=pltpu.CompilerParams(vmem_limit_bytes=GRANT_EXTRA),
    )(hu, hd, par, sta, vg, vown)
    flat = lambda v: v.reshape(-1)
    return hu, hd, hn, hb, nu, nd.T, flat(nn), flat(nb), tu, td.T, flat(tn), flat(tb)


def plain(slope_up, slope_down, slope_norm, slope_bias, param_up, param_down, param_norm, param_bias,
          state_up, state_down, state_norm, state_bias):
    rate = lax.axis_size("dp") ** (-0.5)
    place = lax.axis_index("dp")

    def step(mean, param, state):
        state_new = hold_rate * state + mean * rate
        return param - learn_rate * state_new, state_new

    def scattered(slope, dim):
        return lax.psum_scatter(slope[0].astype(BF16), "dp", scatter_dimension=dim, tiled=True).astype(F32)

    def gathered(value, dim):
        return lax.all_gather(value.astype(BF16), "dp", axis=dim, tiled=True)

    sums = lax.psum((slope_norm[0], slope_bias[0]), "dp")
    size = param_norm.shape[0]
    own = [lax.dynamic_slice_in_dim(v, place * size, size) for v in sums]
    nu, tu = step(scattered(slope_up, 0), param_up, state_up)
    nd, td = step(scattered(slope_down, 1), param_down, state_down)
    nn, tn = step(own[0], param_norm, state_norm)
    nb, tb = step(own[1], param_bias, state_bias)
    halves = gathered(nu, 0), gathered(nd, 1), gathered(nn, 0), gathered(nb, 0)
    return halves + (nu, nd, nn, nb, tu, td, tn, tb)


def body(*args):
    replicas = lax.axis_size("dp")
    chunk, columns = args[4].shape
    fits = replicas == 2 ** 3 and chunk % 16 == 0 and columns % (2 * LANES) == 0
    fits = fits and (replicas * chunk) % LANES == 0
    return (fused if fits else plain)(*args)


def solution(mesh):
    matrices = (P("dp", "tp"), P("tp", "dp"), P("dp"), P("dp"))
    return jax.shard_map(
        body,
        mesh=mesh,
        in_specs=(P("dp", None, "tp"), P("dp", "tp", None), P("dp", None), P("dp", None)) + matrices * 2,
        out_specs=(P(None, "tp"), P("tp", None), P(), P()) + matrices * 2,
        check_vma=False,
    )
```

```python
import functools
import math

import jax
import jax.numpy as jnp
from jax import lax
from jax.experimental import pallas as pl
from jax.experimental.pallas import tpu as pltpu
from jax.sharding import PartitionSpec as P

learn_rate = 0.1
hold_rate = 0.7
LANES = 128
GRANT_EXTRA = 2 * 1024 * 1024
F32 = jnp.float32
BF16 = jnp.bfloat16
FAR, NEAR, RS1, RS2, AG1, AG2, SH1, SH2, END, OVER = range(10)


def widths_of(half, small):
    if half < 2:
        return [half]
    if small:
        return [1] + widths_of(half - 1, False)
    return [half - half // 2, half // 2]


def slab_plan(columns):
    half = columns // LANES // 2
    slabs = []
    for m in (0, 1):
        start = 0
        for width in widths_of(half, m == 0):
            for axis in (0, 1):
                slabs.append((m, start, width * LANES, axis))
                start += width * LANES
    return slabs


def spot(k):
    y, x, core = k // 4, (k // 2) % 2, k % 2
    return (x, y, core) if core else (y, x, core)


def row_loop(rows, step, fn):
    def go(i, carry):
        fn(pl.ds(pl.multiple_of(i * step, step), step))
        return carry

    lax.fori_loop(0, rows // step, go, 0)


def kernel(
    replicas, slabs, order,
    su, sd, sn, sb, pu, pd, pn, pb, tu, td, tn, tb,
    gu, hd, par, sta, vg, vown,
    fu, fd, bu, bd, r0, r1, r2, gd, vin, vpar, vsta, vb, vr0, vr1, vr2,
    send_sem, recv_sem, vsend_sem, vrecv_sem, load_sem, par_sem, vec_sem,
):
    chunk, columns = pu.shape
    width = replicas * chunk
    me = lax.axis_index("dp")
    c = lax.rem(me, 2)
    x = lax.rem(me // 2, 2)
    y = me // 4
    mate = me + 1 - 2 * c
    x_peer, y_peer = me + 2 - 4 * x, me + 4 - 8 * y
    slow, fast = y + c * (x - y), x + c * (y - x)
    nbr = (x_peer + c * (y_peer - x_peer), y_peer + c * (x_peer - y_peer))
    rate = replicas ** (-0.5)
    step = 32 if chunk % 32 == 0 else 16
    count = len(slabs)
    per = len([s for s in slabs if s[0] == 0])
    b, g = (bu, bd), (gu, gd)
    V = count

    over = tuple(peer + 1 - 2 * c for peer in nbr)
    kept = chunk - chunk * 4 // 10 // 16 * 16

    barrier = pltpu.get_barrier_semaphore()
    for peer in (mate,) + nbr:
        pl.semaphore_signal(barrier, inc=1, device_id={"dp": peer}, device_id_type=pl.DeviceIdType.MESH)

    def local(src, dst, sem):
        cp = pltpu.make_async_copy(src, dst, sem)
        cp.start()
        return cp

    loads = {}
    for i, (m, lo, w, axis) in enumerate(slabs):
        if i > 3 and axis == 1:
            continue
        span = pl.ds(lo, w if i < 4 else 2 * w)
        if m == 0:
            loads[i] = local(su.at[0, :, span], fu.at[:, span], load_sem.at[len(loads)])
        else:
            loads[i] = local(sd.at[0, span], fd.at[span], load_sem.at[len(loads)])
    for n, (whole, pair) in enumerate(((vin, (sn, sb)), (vpar, (pn, pb)), (vsta, (tn, tb)))):
        for row in (0, 1):
            local(pair[row], whole.at[row], vec_sem.at[n])
    for n, (whole, pair) in enumerate(((par, (pu, pd)), (sta, (tu, td)))):
        for m in (0, 1):
            local(pair[m], whole.at[m], par_sem.at[n])

    def loaded(sem, *wholes):
        for n, whole in enumerate(wholes):
            pltpu.make_async_copy(whole, whole, sem.at[n]).wait()

    def convert(i):
        m, lo, w, _ = slabs[i]
        if i in loads:
            loads[i].wait()
        if m == 0:
            for k in range(replicas):
                bu[*spot(k), :, lo : lo + w] = fu[k * chunk : (k + 1) * chunk, lo : lo + w].astype(BF16)
        else:
            for block in range(width // LANES):
                first = block * LANES
                turned = fd[lo : lo + w, first : first + LANES].T.astype(BF16)
                done = 0
                while done < LANES:
                    k, off = divmod(first + done, chunk)
                    n = min(LANES - done, chunk - off)
                    bd[*spot(k), off : off + n, lo : lo + w] = turned[done : done + n]
                    done += n

    leave = {FAR: 0, NEAR: 0, AG2: 1, END: 1, SH1: 1, RS1: 2, SH2: 2, OVER: 2, RS2: 3, AG1: 3}
    vec_out = {FAR: 0, AG2: 0, SH1: 0, RS1: 1, SH2: 1, RS2: 2, AG1: 2}
    vec_in = {FAR: 0, AG1: 0, RS1: 1, AG2: 4, RS2: 2, SH1: 3, SH2: 3}

    def arrival(i, kind):
        if kind in (SH1, SH2, OVER):
            return 3 * count + (1 + (i - per) // 2 if slabs[i][0] else 0)
        if kind in (NEAR, END):
            return 3 * count + 1 + (count - per) // 2 + (kind == END)
        return {FAR: 0, AG1: 0, RS1: 1, AG2: 1, RS2: 2}[kind] * count + (i ^ 1 if kind == AG2 else i)

    def remote(i, kind, src, dst, target):
        if i == V:
            sems = vsend_sem.at[vec_out[kind]], vrecv_sem.at[vec_in[kind]]
        else:
            sems = send_sem.at[leave[kind]], recv_sem.at[arrival(i, kind)]
        return pltpu.make_async_remote_copy(
            src_ref=src, dst_ref=dst, send_sem=sems[0], recv_sem=sems[1],
            device_id={"dp": target}, device_id_type=pl.DeviceIdType.MESH,
        )

    copies = {}

    def copy(i, kind, src, dst, target):
        copies[i, kind] = remote(i, kind, src, dst, target)
        copies[i, kind].start()

    def sent(kind, whole):
        remote(0, kind, whole, whole, mate).wait_send()

    def swap(i, kind):
        m, lo, w, axis = slabs[i]
        cols = pl.ds(lo, w)
        if axis == 0:
            at = 1 - slow if kind == FAR else slow
            copy(i, kind, b[m].at[:, at, 1 - c, :, cols], r0.at[m, :, at, :, cols], mate)
        else:
            at = 1 - fast if kind == FAR else fast
            copy(i, kind, b[m].at[at, :, 1 - c, :, cols], r0.at[m, at, :, :, cols], mate)

    def rs1(i):
        m, lo, w, axis = slabs[i]
        cols = pl.ds(lo, w)
        copies[i, FAR].wait_recv()
        for j in (0, 1):
            at = (j, 1 - fast) if axis == 0 else (1 - slow, j)
            b[m][*at, c, :, lo : lo + w] = b[m][*at, c, :, lo : lo + w] + r0[m, *at, :, lo : lo + w]
        src = b[m].at[:, 1 - fast, c, :, cols] if axis == 0 else b[m].at[1 - slow, :, c, :, cols]
        copy(i, RS1, src, r1.at[m, :, :, cols], nbr[axis])

    def rs2(i):
        m, lo, w, axis = slabs[i]
        cs = slice(lo, lo + w)
        cols = pl.ds(lo, w)
        copies[i, RS1].wait_recv()
        j = 1 - slow if axis == 0 else 1 - fast
        far = (1 - slow, fast) if axis == 0 else (slow, 1 - fast)
        b[m][*far, c, :, cs] = b[m][*far, c, :, cs] + r0[m, *far, :, cs] + r1[m, j, :, cs]
        copy(i, RS2, b[m].at[*far, c, :, cols], r2.at[m, :, cols], nbr[1 - axis])
        own = slow, fast
        b[m][*own, c, :, cs] = b[m][*own, c, :, cs] + r0[m, *own, :, cs] + r1[m, 1 - j, :, cs]

    def update(i):
        m, lo, w, axis = slabs[i]
        cs = slice(lo, lo + w)
        cols = pl.ds(lo, w)
        copies[i, RS2].wait_recv()
        own, out = b[m].at[slow, fast, c], g[m].at[slow, fast, c]

        def go(rows):
            mean = (own[rows, cs].astype(F32) + r2[m, rows, cs].astype(F32)) * rate
            state = hold_rate * sta[m, rows, cs] + mean
            new = par[m, rows, cs] - learn_rate * state
            out[rows, cs] = new.astype(BF16)
            sta[m, rows, cs] = state
            par[m, rows, cs] = new

        row_loop(chunk, step, go)
        copy(i, AG1, out.at[:, cols], out.at[:, cols], nbr[1 - axis])

    def ag2(i):
        m, lo, w, axis = slabs[i]
        cols = pl.ds(lo, w)
        copies[i, AG1].wait_recv()
        part = g[m].at[:, fast, c] if axis == 0 else g[m].at[slow, :, c]
        early = part.at[:, pl.ds(0, kept if i < 2 else chunk), cols]
        copy(i, AG2, early, early, nbr[axis])
        copy(i, SH1, part.at[:, :, cols], part.at[:, :, cols], mate)

    def ends():
        for i in (0, 1):
            m, lo, w, axis = slabs[i]
            part = g[m].at[:, fast, c] if axis == 0 else g[m].at[slow, :, c]
            rest = part.at[:, pl.ds(kept, chunk - kept), pl.ds(lo, w)]
            copy(i, END, rest, rest, nbr[axis])
            copy(i, OVER, rest, rest, over[axis])

    def share(i):
        m, lo, w, axis = slabs[i]
        cols = pl.ds(lo, w)
        copies[i, AG2].wait_recv()
        part = g[m].at[:, 1 - fast, c] if axis == 0 else g[m].at[1 - slow, :, c]
        part = part.at[:, pl.ds(0, kept if i < 2 else chunk), cols]
        copy(i, SH2, part, part, mate)

    def finish(i):
        m, lo, w, axis = slabs[i]
        if m == 1:
            if axis == 0:
                pair = gd.at[:, :, 1 - c, :, pl.ds(lo, 2 * w)]
                remote(i, SH2, pair, pair, mate).wait_recv()
            for block in range(width // LANES):
                first, done, parts = block * LANES, 0, []
                while done < LANES:
                    k, off = divmod(first + done, chunk)
                    n = min(LANES - done, chunk - off)
                    parts.append(gd[*spot(k), off : off + n, lo : lo + w].astype(F32))
                    done += n
                whole = parts[0] if len(parts) == 1 else jnp.concatenate(parts, axis=0)
                hd[lo : lo + w, first : first + LANES] = whole.T.astype(BF16)

    def vec_swap():
        loaded(vec_sem, vin, vpar, vsta)
        for row in (0, 1):
            for k in range(replicas):
                vb[*spot(k), row : row + 1, 0:chunk] = vin[row, :, k * chunk : (k + 1) * chunk]
        copy(V, FAR, vb.at[:, :, 1 - c], vr0, mate)

    def vec_rs1():
        copies[V, FAR].wait_recv()
        for at in ((0, 0), (0, 1), (1, 0), (1, 1)):
            vb[*at, c] = vb[*at, c] + vr0[*at]
        copy(V, RS1, vb.at[:, 1 - fast, c], vr1, nbr[0])

    def vec_rs2():
        copies[V, RS1].wait_recv()
        for j in (0, 1):
            vb[j, fast, c] = vb[j, fast, c] + vr1[j]
        copy(V, RS2, vb.at[1 - slow, fast, c], vr2, nbr[1])

    def vec_update():
        copies[V, RS2].wait_recv()
        mean = (vb[slow, fast, c] + vr2[...]) * rate
        for row in (0, 1):
            state = hold_rate * vsta[row] + mean[row : row + 1, 0:chunk]
            new = vpar[row] - learn_rate * state
            vg[slow, fast, c, row : row + 1, 0:chunk] = new
            vown[row] = new
            vown[2 + row] = state
        copy(V, AG1, vg.at[slow, fast, c], vg.at[slow, fast, c], nbr[1])

    def vec_ag2():
        copies[V, AG1].wait_recv()
        part = vg.at[:, fast, c]
        copy(V, AG2, part, part, nbr[0])
        copy(V, SH1, part, part, mate)

    def vec_share():
        copies[V, AG2].wait_recv()
        part = vg.at[:, 1 - fast, c]
        copy(V, SH2, part, part, mate)

    vb[...] = jnp.zeros_like(vb)
    vg[slow, fast, c] = jnp.zeros(vr2.shape, F32)
    convert(0)
    pl.semaphore_wait(barrier, 3)
    swap(0, FAR)
    convert(1)
    swap(1, FAR)
    rs1(0)
    rs1(1)
    for i in range(2, count):
        convert(i)
        swap(i, FAR)
        if i > 3:
            rs1(i - 2)
        if i == 6:
            vec_swap()
        if i == 8:
            vec_rs1()
    for i in (count - 2, count - 1):
        rs1(i)
    for i in range(count):
        swap(i, NEAR)
    remote(0, NEAR, r1, r1, mate).wait_recv()

    for i in range(count):
        rs2(i)
        if i == 4:
            sent(FAR, r0)
        if i == 7:
            vec_rs2()
    loaded(par_sem, par, sta)
    for n, i in enumerate(list(range(2, count)) + [0, 1]):
        update(i)
        if n == 6:
            vec_update()
    for n, i in enumerate(order):
        ag2(i)
        if n == 4:
            vec_ag2()
    ends()
    for n, i in enumerate(order):
        share(i)
        if n == 0:
            sent(RS2, r1)
        if n == 5:
            vec_share()
        if n > 1:
            finish(order[n - 2])
    finish(order[-2])
    finish(order[-1])
    other = vg.at[:, :, 1 - c]
    remote(V, SH2, other, other, mate).wait_recv()
    for whole, kind in ((vb, FAR), (vr0, RS1), (vr1, RS2)):
        remote(V, kind, whole, whole, mate).wait_send()
    rest = gu.at[:, 0, c, pl.ds(kept, chunk - kept), pl.ds(0, 2 * slabs[0][2])]
    remote(0, END, rest, rest, mate).wait_recv()
    whole = gu.at[:, :, 1 - c]
    remote(0, SH2, whole, whole, mate).wait_recv()
    sent(AG2, r0)
    sent(SH2, r0)


def spill(
    replicas, chunk,
    hu, hd, par, sta, vg, vown,
    hu_out, hd_out, nu_out, nd_out, tu_out, td_out, nn_out, nb_out, tn_out, tb_out, hn_out, hb_out,
    hv0, hv1, sem,
):
    width = replicas * chunk
    vw = columns_pad(chunk)
    for k in range(replicas):
        pltpu.make_async_copy(hu.at[*spot(k)], hu_out.at[pl.ds(k * chunk, chunk)], sem.at[0]).start()
    moves = [
        (hd, hd_out), (par.at[0], nu_out), (par.at[1], nd_out), (sta.at[0], tu_out), (sta.at[1], td_out),
        (vown.at[0], nn_out), (vown.at[1], nb_out), (vown.at[2], tn_out), (vown.at[3], tb_out),
        (hv0, hn_out), (hv1, hb_out),
    ]
    stores = [pltpu.make_async_copy(src, dst, sem.at[i + 1]) for i, (src, dst) in enumerate(moves)]
    for cp in stores[:-2]:
        cp.start()
    lane = lax.broadcasted_iota(jnp.int32, (2, width), 1)
    full = jnp.zeros((2, width), F32)
    for k in range(replicas):
        piece = vg[*spot(k)]
        wide = jnp.concatenate([piece, jnp.zeros((2, width - vw), F32)], axis=1) if width > vw else piece
        moved = pltpu.roll(wide, k * chunk, 1) if k else wide
        full = jnp.where((lane >= k * chunk) & (lane < (k + 1) * chunk), moved, full)
    for row, out in enumerate((hv0, hv1)):
        out[...] = full[row].astype(BF16)
    for cp in stores[-2:]:
        cp.start()
    for cp in stores:
        cp.wait()
    pltpu.make_async_copy(hu_out, hu_out, sem.at[0]).wait()


def columns_pad(n):
    return -(-n // LANES) * LANES


def fused(slope_up, slope_down, slope_norm, slope_bias, param_up, param_down, param_norm, param_bias,
          state_up, state_down, state_norm, state_bias):
    replicas = lax.axis_size("dp")
    chunk, columns = param_up.shape
    width = replicas * chunk
    slabs = slab_plan(columns)
    count = len(slabs)
    per = len([s for s in slabs if s[0] == 0])
    order = list(range(2, 4)) + list(range(per, count)) + list(range(4, per)) + [0, 1]
    vw = columns_pad(chunk)
    hbm = pl.BlockSpec(memory_space=pl.ANY)
    vmem = pl.BlockSpec(memory_space=pltpu.VMEM)
    cube = (2, 2, 2, chunk, columns)
    shape = jax.ShapeDtypeStruct
    dma = pltpu.SemaphoreType.DMA
    row = lambda v: v.reshape(1, -1)
    scratch = [
        pltpu.VMEM((width, columns), F32), pltpu.VMEM((columns, width), F32),
        pltpu.VMEM(cube, BF16), pltpu.VMEM(cube, BF16),
        pltpu.VMEM((2, 2, 2, chunk, columns), BF16),
        pltpu.VMEM((2, 2, chunk, columns), BF16),
        pltpu.VMEM((2, chunk, columns), BF16),
        pltpu.VMEM(cube, BF16),
        pltpu.VMEM((2, 1, width), F32), pltpu.VMEM((2, 1, chunk), F32), pltpu.VMEM((2, 1, chunk), F32),
        pltpu.VMEM((2, 2, 2, 2, vw), F32), pltpu.VMEM((2, 2, 2, vw), F32),
        pltpu.VMEM((2, 2, vw), F32), pltpu.VMEM((2, vw), F32),
    ]
    grant = sum(math.prod(s.shape) * jnp.dtype(s.dtype).itemsize for s in scratch) + GRANT_EXTRA
    hu, hd, par, sta, vg, vown = pl.pallas_call(
        functools.partial(kernel, replicas, slabs, order),
        out_shape=(
            pltpu.VMEM(cube, BF16), pltpu.VMEM((columns, width), BF16),
            pltpu.VMEM((2, chunk, columns), F32), pltpu.VMEM((2, chunk, columns), F32),
            pltpu.VMEM((2, 2, 2, 2, vw), F32), pltpu.VMEM((4, 1, chunk), F32),
        ),
        in_specs=[hbm] * 12,
        out_specs=[vmem] * 6,
        scratch_shapes=scratch + [
            dma((4,)), dma((3 * count + 3 + (count - per) // 2,)), dma((3,)), dma((5,)),
            dma((2 + count // 2,)), dma((2,)), dma((3,)),
        ],
        compiler_params=pltpu.CompilerParams(collective_id=0, has_side_effects=True, vmem_limit_bytes=grant),
    )(*(pltpu.with_memory_space_constraint(v, pltpu.HBM) for v in (
        slope_up, slope_down, slope_norm, slope_bias,
        param_up, param_down.T, row(param_norm), row(param_bias),
        state_up, state_down.T, row(state_norm), row(state_bias),
    )))
    block, line = shape((chunk, columns), F32), shape((1, chunk), F32)
    half = shape((width,), BF16)
    hu, hd, nu, nd, tu, td, nn, nb, tn, tb, hn, hb = pl.pallas_call(
        functools.partial(spill, replicas, chunk),
        out_shape=(shape((width, columns), BF16), shape((columns, width), BF16)) + (block,) * 4 + (line,) * 4 + (half,) * 2,
        in_specs=[vmem] * 6,
        out_specs=[hbm] * 12,
        scratch_shapes=[pltpu.VMEM((width,), BF16), pltpu.VMEM((width,), BF16), dma((12,))],
        compiler_params=pltpu.CompilerParams(vmem_limit_bytes=GRANT_EXTRA),
    )(hu, hd, par, sta, vg, vown)
    flat = lambda v: v.reshape(-1)
    return hu, hd, hn, hb, nu, nd.T, flat(nn), flat(nb), tu, td.T, flat(tn), flat(tb)


def plain(slope_up, slope_down, slope_norm, slope_bias, param_up, param_down, param_norm, param_bias,
          state_up, state_down, state_norm, state_bias):
    rate = lax.axis_size("dp") ** (-0.5)
    place = lax.axis_index("dp")

    def step(mean, param, state):
        state_new = hold_rate * state + mean * rate
        return param - learn_rate * state_new, state_new

    def scattered(slope, dim):
        return lax.psum_scatter(slope[0].astype(BF16), "dp", scatter_dimension=dim, tiled=True).astype(F32)

    def gathered(value, dim):
        return lax.all_gather(value.astype(BF16), "dp", axis=dim, tiled=True)

    sums = lax.psum((slope_norm[0], slope_bias[0]), "dp")
    size = param_norm.shape[0]
    own = [lax.dynamic_slice_in_dim(v, place * size, size) for v in sums]
    nu, tu = step(scattered(slope_up, 0), param_up, state_up)
    nd, td = step(scattered(slope_down, 1), param_down, state_down)
    nn, tn = step(own[0], param_norm, state_norm)
    nb, tb = step(own[1], param_bias, state_bias)
    halves = gathered(nu, 0), gathered(nd, 1), gathered(nn, 0), gathered(nb, 0)
    return halves + (nu, nd, nn, nb, tu, td, tn, tb)


def body(*args):
    replicas = lax.axis_size("dp")
    chunk, columns = args[4].shape
    fits = replicas == 2 ** 3 and chunk % 16 == 0 and columns % (2 * LANES) == 0
    fits = fits and (replicas * chunk) % LANES == 0
    return (fused if fits else plain)(*args)


def solution(mesh):
    matrices = (P("dp", "tp"), P("tp", "dp"), P("dp"), P("dp"))
    return jax.shard_map(
        body,
        mesh=mesh,
        in_specs=(P("dp", None, "tp"), P("dp", "tp", None), P("dp", None), P("dp", None)) + matrices * 2,
        out_specs=(P(None, "tp"), P("tp", None), P(), P()) + matrices * 2,
        check_vma=False,
    )
```

```python
import functools
import math

import jax
import jax.numpy as jnp
from jax import lax
from jax.experimental import pallas as pl
from jax.experimental.pallas import tpu as pltpu
from jax.sharding import PartitionSpec as P

learn_rate = 0.1
hold_rate = 0.7
LANES = 128
GRANT_EXTRA = 2 * 1024 * 1024
F32 = jnp.float32
BF16 = jnp.bfloat16
FAR, NEAR, RS1, RS2, AG1, AG2, SH1, SH2, END, OVER = range(10)


def widths_of(half, small):
    if half < 2:
        return [half]
    if small:
        return [1] + widths_of(half - 1, False)
    return [half - half // 2, half // 2]


def slab_plan(columns):
    half = columns // LANES // 2
    slabs = []
    for m in (0, 1):
        start = 0
        for width in widths_of(half, m == 0):
            for axis in (0, 1):
                slabs.append((m, start, width * LANES, axis))
                start += width * LANES
    return slabs


def spot(k):
    y, x, core = k // 4, (k // 2) % 2, k % 2
    return (x, y, core) if core else (y, x, core)


def row_loop(rows, step, fn):
    def go(i, carry):
        fn(pl.ds(pl.multiple_of(i * step, step), step))
        return carry

    lax.fori_loop(0, rows // step, go, 0)


def kernel(
    replicas, slabs, order,
    su, sd, sn, sb, pu, pd, pn, pb, tu, td, tn, tb,
    gu, hd, par, sta, vg, vown,
    fu, fd, bu, bd, r0, r1, r2, gd, vin, vpar, vsta, vb, vr0, vr1, vr2,
    send_sem, recv_sem, vsend_sem, vrecv_sem, load_sem, par_sem, vec_sem,
):
    chunk, columns = pu.shape
    width = replicas * chunk
    me = lax.axis_index("dp")
    c = lax.rem(me, 2)
    x = lax.rem(me // 2, 2)
    y = me // 4
    mate = me + 1 - 2 * c
    x_peer, y_peer = me + 2 - 4 * x, me + 4 - 8 * y
    slow, fast = y + c * (x - y), x + c * (y - x)
    nbr = (x_peer + c * (y_peer - x_peer), y_peer + c * (x_peer - y_peer))
    rate = replicas ** (-0.5)
    step = 32 if chunk % 32 == 0 else 16
    count = len(slabs)
    per = len([s for s in slabs if s[0] == 0])
    b, g = (bu, bd), (gu, gd)
    V = count

    over = tuple(peer + 1 - 2 * c for peer in nbr)
    kept = chunk - chunk * 4 // 10 // 16 * 16

    barrier = pltpu.get_barrier_semaphore()
    for peer in (mate,) + nbr:
        pl.semaphore_signal(barrier, inc=1, device_id={"dp": peer}, device_id_type=pl.DeviceIdType.MESH)

    def local(src, dst, sem):
        cp = pltpu.make_async_copy(src, dst, sem)
        cp.start()
        return cp

    loads = {}
    for i, (m, lo, w, axis) in enumerate(slabs):
        if i > 3 and axis == 1:
            continue
        span = pl.ds(lo, w if i < 4 else 2 * w)
        if m == 0:
            loads[i] = local(su.at[0, :, span], fu.at[:, span], load_sem.at[len(loads)])
        else:
            loads[i] = local(sd.at[0, span], fd.at[span], load_sem.at[len(loads)])
    for n, (whole, pair) in enumerate(((vin, (sn, sb)), (vpar, (pn, pb)), (vsta, (tn, tb)))):
        for row in (0, 1):
            local(pair[row], whole.at[row], vec_sem.at[n])
    for n, (whole, pair) in enumerate(((par, (pu, pd)), (sta, (tu, td)))):
        for m in (0, 1):
            local(pair[m], whole.at[m], par_sem.at[n])

    def loaded(sem, *wholes):
        for n, whole in enumerate(wholes):
            pltpu.make_async_copy(whole, whole, sem.at[n]).wait()

    def convert(i):
        m, lo, w, _ = slabs[i]
        if i in loads:
            loads[i].wait()
        if m == 0:
            for k in range(replicas):
                bu[*spot(k), :, lo : lo + w] = fu[k * chunk : (k + 1) * chunk, lo : lo + w].astype(BF16)
        else:
            for block in range(width // LANES):
                first = block * LANES
                turned = fd[lo : lo + w, first : first + LANES].T.astype(BF16)
                done = 0
                while done < LANES:
                    k, off = divmod(first + done, chunk)
                    n = min(LANES - done, chunk - off)
                    bd[*spot(k), off : off + n, lo : lo + w] = turned[done : done + n]
                    done += n

    leave = {FAR: 0, NEAR: 0, AG2: 1, END: 1, SH1: 1, RS1: 2, SH2: 2, OVER: 2, RS2: 3, AG1: 3}
    vec_out = {FAR: 0, AG2: 0, SH1: 0, RS1: 1, SH2: 1, RS2: 2, AG1: 2}
    vec_in = {FAR: 0, AG1: 0, RS1: 1, AG2: 4, RS2: 2, SH1: 3, SH2: 3}

    half = count // 2

    def arrival(i, kind):
        if kind in (SH1, SH2, OVER):
            return 2 * count + (1 + (i - per) // 2 if slabs[i][0] else 0)
        if kind in (NEAR, END):
            return 2 * count + 1 + (count - per) // 2 + (kind == END)
        return i if kind in (FAR, AG1) else count + i // 2 + (half if kind == RS2 else 0)

    def remote(i, kind, src, dst, target):
        if i == V:
            sems = vsend_sem.at[vec_out[kind]], vrecv_sem.at[vec_in[kind]]
        else:
            sems = send_sem.at[leave[kind]], recv_sem.at[arrival(i, kind)]
        return pltpu.make_async_remote_copy(
            src_ref=src, dst_ref=dst, send_sem=sems[0], recv_sem=sems[1],
            device_id={"dp": target}, device_id_type=pl.DeviceIdType.MESH,
        )

    copies = {}

    def arrived(i, kind):
        m, lo, w, axis = slabs[i]
        if axis:
            return
        cols = pl.ds(lo, 2 * w)
        if kind == RS2:
            whole = r2.at[m, :, cols]
        else:
            whole = r1.at[m, :, pl.ds(0, kept if kind == AG2 and i < 2 else chunk), cols]
        remote(i, kind, whole, whole, mate).wait_recv()

    def copy(i, kind, src, dst, target):
        copies[i, kind] = remote(i, kind, src, dst, target)
        copies[i, kind].start()

    def sent(kind, whole):
        remote(0, kind, whole, whole, mate).wait_send()

    def swap(i, kind):
        m, lo, w, axis = slabs[i]
        cols = pl.ds(lo, w)
        if axis == 0:
            at = 1 - slow if kind == FAR else slow
            copy(i, kind, b[m].at[:, at, 1 - c, :, cols], r0.at[m, :, at, :, cols], mate)
        else:
            at = 1 - fast if kind == FAR else fast
            copy(i, kind, b[m].at[at, :, 1 - c, :, cols], r0.at[m, at, :, :, cols], mate)

    def rs1(i):
        m, lo, w, axis = slabs[i]
        cols = pl.ds(lo, w)
        copies[i, FAR].wait_recv()
        for j in (0, 1):
            at = (j, 1 - fast) if axis == 0 else (1 - slow, j)
            b[m][*at, c, :, lo : lo + w] = b[m][*at, c, :, lo : lo + w] + r0[m, *at, :, lo : lo + w]
        src = b[m].at[:, 1 - fast, c, :, cols] if axis == 0 else b[m].at[1 - slow, :, c, :, cols]
        copy(i, RS1, src, r1.at[m, :, :, cols], nbr[axis])

    def rs2(i):
        m, lo, w, axis = slabs[i]
        cs = slice(lo, lo + w)
        cols = pl.ds(lo, w)
        arrived(i, RS1)
        j = 1 - slow if axis == 0 else 1 - fast
        far = (1 - slow, fast) if axis == 0 else (slow, 1 - fast)
        b[m][*far, c, :, cs] = b[m][*far, c, :, cs] + r0[m, *far, :, cs] + r1[m, j, :, cs]
        copy(i, RS2, b[m].at[*far, c, :, cols], r2.at[m, :, cols], nbr[1 - axis])
        own = slow, fast
        b[m][*own, c, :, cs] = b[m][*own, c, :, cs] + r0[m, *own, :, cs] + r1[m, 1 - j, :, cs]

    def update(i):
        m, lo, w, axis = slabs[i]
        cs = slice(lo, lo + w)
        cols = pl.ds(lo, w)
        arrived(i, RS2)
        own, out = b[m].at[slow, fast, c], g[m].at[slow, fast, c]

        def go(rows):
            mean = (own[rows, cs].astype(F32) + r2[m, rows, cs].astype(F32)) * rate
            state = hold_rate * sta[m, rows, cs] + mean
            new = par[m, rows, cs] - learn_rate * state
            out[rows, cs] = new.astype(BF16)
            sta[m, rows, cs] = state
            par[m, rows, cs] = new

        row_loop(chunk, step, go)
        copy(i, AG1, out.at[:, cols], out.at[:, cols], nbr[1 - axis])

    def ag2(i):
        m, lo, w, axis = slabs[i]
        cols = pl.ds(lo, w)
        copies[i, AG1].wait_recv()
        part = g[m].at[:, fast, c] if axis == 0 else g[m].at[slow, :, c]
        early = part.at[:, pl.ds(0, kept if i < 2 else chunk), cols]
        copy(i, AG2, early, early, nbr[axis])
        copy(i, SH1, part.at[:, :, cols], part.at[:, :, cols], mate)

    def ends():
        for i in (0, 1):
            m, lo, w, axis = slabs[i]
            part = g[m].at[:, fast, c] if axis == 0 else g[m].at[slow, :, c]
            rest = part.at[:, pl.ds(kept, chunk - kept), pl.ds(lo, w)]
            copy(i, END, rest, rest, nbr[axis])
            copy(i, OVER, rest, rest, over[axis])

    def share(i):
        m, lo, w, axis = slabs[i]
        cols = pl.ds(lo, w)
        arrived(i, AG2)
        part = g[m].at[:, 1 - fast, c] if axis == 0 else g[m].at[1 - slow, :, c]
        part = part.at[:, pl.ds(0, kept if i < 2 else chunk), cols]
        copy(i, SH2, part, part, mate)

    def finish(i):
        m, lo, w, axis = slabs[i]
        if m == 1:
            if axis == 0:
                pair = gd.at[:, :, 1 - c, :, pl.ds(lo, 2 * w)]
                remote(i, SH2, pair, pair, mate).wait_recv()
            for block in range(width // LANES):
                first, done, parts = block * LANES, 0, []
                while done < LANES:
                    k, off = divmod(first + done, chunk)
                    n = min(LANES - done, chunk - off)
                    parts.append(gd[*spot(k), off : off + n, lo : lo + w].astype(F32))
                    done += n
                whole = parts[0] if len(parts) == 1 else jnp.concatenate(parts, axis=0)
                hd[lo : lo + w, first : first + LANES] = whole.T.astype(BF16)

    def vec_swap():
        loaded(vec_sem, vin, vpar, vsta)
        for row in (0, 1):
            for k in range(replicas):
                vb[*spot(k), row : row + 1, 0:chunk] = vin[row, :, k * chunk : (k + 1) * chunk]
        copy(V, FAR, vb.at[:, :, 1 - c], vr0, mate)

    def vec_rs1():
        copies[V, FAR].wait_recv()
        for at in ((0, 0), (0, 1), (1, 0), (1, 1)):
            vb[*at, c] = vb[*at, c] + vr0[*at]
        copy(V, RS1, vb.at[:, 1 - fast, c], vr1, nbr[0])

    def vec_rs2():
        copies[V, RS1].wait_recv()
        for j in (0, 1):
            vb[j, fast, c] = vb[j, fast, c] + vr1[j]
        copy(V, RS2, vb.at[1 - slow, fast, c], vr2, nbr[1])

    def vec_update():
        copies[V, RS2].wait_recv()
        mean = (vb[slow, fast, c] + vr2[...]) * rate
        for row in (0, 1):
            state = hold_rate * vsta[row] + mean[row : row + 1, 0:chunk]
            new = vpar[row] - learn_rate * state
            vg[slow, fast, c, row : row + 1, 0:chunk] = new
            vown[row] = new
            vown[2 + row] = state
        copy(V, AG1, vg.at[slow, fast, c], vg.at[slow, fast, c], nbr[1])

    def vec_ag2():
        copies[V, AG1].wait_recv()
        part = vg.at[:, fast, c]
        copy(V, AG2, part, part, nbr[0])
        copy(V, SH1, part, part, mate)

    def vec_share():
        copies[V, AG2].wait_recv()
        part = vg.at[:, 1 - fast, c]
        copy(V, SH2, part, part, mate)

    vb[...] = jnp.zeros_like(vb)
    vg[slow, fast, c] = jnp.zeros(vr2.shape, F32)
    convert(0)
    pl.semaphore_wait(barrier, 3)
    swap(0, FAR)
    convert(1)
    swap(1, FAR)
    rs1(0)
    rs1(1)
    for i in range(2, count):
        if i == 4:
            rs1(2)
        convert(i)
        swap(i, FAR)
        if i > 4:
            rs1(i - 2)
        if i == 6:
            vec_swap()
        if i == 8:
            vec_rs1()
    for i in (count - 2, count - 1):
        rs1(i)
    for i in range(count):
        swap(i, NEAR)
    remote(0, NEAR, r1, r1, mate).wait_recv()

    for i in range(count):
        rs2(i)
        if i == 4:
            sent(FAR, r0)
        if i == 7:
            vec_rs2()
    loaded(par_sem, par, sta)
    for n, i in enumerate(list(range(2, count)) + [0, 1]):
        update(i)
        if n == 6:
            vec_update()
    for n, i in enumerate(order):
        ag2(i)
        if n == 4:
            vec_ag2()
    ends()
    for n, i in enumerate(order):
        share(i)
        if n == 0:
            sent(RS2, r1)
        if n == 5:
            vec_share()
        if n == count - 2:
            other = vg.at[:, :, 1 - c]
            remote(V, SH2, other, other, mate).wait_recv()
            for whole, kind in ((vb, FAR), (vr0, RS1), (vr1, RS2)):
                remote(V, kind, whole, whole, mate).wait_send()
        if n > 1:
            finish(order[n - 2])
    finish(order[-2])
    finish(order[-1])
    rest = gu.at[:, 0, c, pl.ds(kept, chunk - kept), pl.ds(0, 2 * slabs[0][2])]
    remote(0, END, rest, rest, mate).wait_recv()
    whole = gu.at[:, :, 1 - c]
    remote(0, SH2, whole, whole, mate).wait_recv()
    sent(AG2, r0)
    sent(SH2, r0)


def spill(
    replicas, chunk,
    hu, hd, par, sta, vg, vown,
    hu_out, hd_out, nu_out, nd_out, tu_out, td_out, nn_out, nb_out, tn_out, tb_out, hn_out, hb_out,
    hv0, hv1, sem,
):
    width = replicas * chunk
    vw = columns_pad(chunk)
    for k in range(replicas):
        pltpu.make_async_copy(hu.at[*spot(k)], hu_out.at[pl.ds(k * chunk, chunk)], sem.at[0]).start()
    moves = [
        (hd, hd_out), (par.at[0], nu_out), (par.at[1], nd_out), (sta.at[0], tu_out), (sta.at[1], td_out),
        (vown.at[0], nn_out), (vown.at[1], nb_out), (vown.at[2], tn_out), (vown.at[3], tb_out),
        (hv0, hn_out), (hv1, hb_out),
    ]
    stores = [pltpu.make_async_copy(src, dst, sem.at[i + 1]) for i, (src, dst) in enumerate(moves)]
    for cp in stores[:-2]:
        cp.start()
    lane = lax.broadcasted_iota(jnp.int32, (2, width), 1)
    full = jnp.zeros((2, width), F32)
    for k in range(replicas):
        piece = vg[*spot(k)]
        wide = jnp.concatenate([piece, jnp.zeros((2, width - vw), F32)], axis=1) if width > vw else piece
        moved = pltpu.roll(wide, k * chunk, 1) if k else wide
        full = jnp.where((lane >= k * chunk) & (lane < (k + 1) * chunk), moved, full)
    for row, out in enumerate((hv0, hv1)):
        out[...] = full[row].astype(BF16)
    for cp in stores[-2:]:
        cp.start()
    for cp in stores:
        cp.wait()
    pltpu.make_async_copy(hu_out, hu_out, sem.at[0]).wait()


def columns_pad(n):
    return -(-n // LANES) * LANES


def fused(slope_up, slope_down, slope_norm, slope_bias, param_up, param_down, param_norm, param_bias,
          state_up, state_down, state_norm, state_bias):
    replicas = lax.axis_size("dp")
    chunk, columns = param_up.shape
    width = replicas * chunk
    slabs = slab_plan(columns)
    count = len(slabs)
    per = len([s for s in slabs if s[0] == 0])
    order = list(range(2, 4)) + list(range(per, count)) + list(range(4, per)) + [0, 1]
    vw = columns_pad(chunk)
    hbm = pl.BlockSpec(memory_space=pl.ANY)
    vmem = pl.BlockSpec(memory_space=pltpu.VMEM)
    cube = (2, 2, 2, chunk, columns)
    shape = jax.ShapeDtypeStruct
    dma = pltpu.SemaphoreType.DMA
    row = lambda v: v.reshape(1, -1)
    scratch = [
        pltpu.VMEM((width, columns), F32), pltpu.VMEM((columns, width), F32),
        pltpu.VMEM(cube, BF16), pltpu.VMEM(cube, BF16),
        pltpu.VMEM((2, 2, 2, chunk, columns), BF16),
        pltpu.VMEM((2, 2, chunk, columns), BF16),
        pltpu.VMEM((2, chunk, columns), BF16),
        pltpu.VMEM(cube, BF16),
        pltpu.VMEM((2, 1, width), F32), pltpu.VMEM((2, 1, chunk), F32), pltpu.VMEM((2, 1, chunk), F32),
        pltpu.VMEM((2, 2, 2, 2, vw), F32), pltpu.VMEM((2, 2, 2, vw), F32),
        pltpu.VMEM((2, 2, vw), F32), pltpu.VMEM((2, vw), F32),
    ]
    grant = sum(math.prod(s.shape) * jnp.dtype(s.dtype).itemsize for s in scratch) + GRANT_EXTRA
    hu, hd, par, sta, vg, vown = pl.pallas_call(
        functools.partial(kernel, replicas, slabs, order),
        out_shape=(
            pltpu.VMEM(cube, BF16), pltpu.VMEM((columns, width), BF16),
            pltpu.VMEM((2, chunk, columns), F32), pltpu.VMEM((2, chunk, columns), F32),
            pltpu.VMEM((2, 2, 2, 2, vw), F32), pltpu.VMEM((4, 1, chunk), F32),
        ),
        in_specs=[hbm] * 12,
        out_specs=[vmem] * 6,
        scratch_shapes=scratch + [
            dma((4,)), dma((2 * count + 3 + (count - per) // 2,)), dma((3,)), dma((5,)),
            dma((2 + count // 2,)), dma((2,)), dma((3,)),
        ],
        compiler_params=pltpu.CompilerParams(collective_id=0, has_side_effects=True, vmem_limit_bytes=grant),
    )(*(pltpu.with_memory_space_constraint(v, pltpu.HBM) for v in (
        slope_up, slope_down, slope_norm, slope_bias,
        param_up, param_down.T, row(param_norm), row(param_bias),
        state_up, state_down.T, row(state_norm), row(state_bias),
    )))
    block, line = shape((chunk, columns), F32), shape((1, chunk), F32)
    half = shape((width,), BF16)
    hu, hd, nu, nd, tu, td, nn, nb, tn, tb, hn, hb = pl.pallas_call(
        functools.partial(spill, replicas, chunk),
        out_shape=(shape((width, columns), BF16), shape((columns, width), BF16)) + (block,) * 4 + (line,) * 4 + (half,) * 2,
        in_specs=[vmem] * 6,
        out_specs=[hbm] * 12,
        scratch_shapes=[pltpu.VMEM((width,), BF16), pltpu.VMEM((width,), BF16), dma((12,))],
        compiler_params=pltpu.CompilerParams(vmem_limit_bytes=GRANT_EXTRA),
    )(hu, hd, par, sta, vg, vown)
    flat = lambda v: v.reshape(-1)
    return hu, hd, hn, hb, nu, nd.T, flat(nn), flat(nb), tu, td.T, flat(tn), flat(tb)


def plain(slope_up, slope_down, slope_norm, slope_bias, param_up, param_down, param_norm, param_bias,
          state_up, state_down, state_norm, state_bias):
    rate = lax.axis_size("dp") ** (-0.5)
    place = lax.axis_index("dp")

    def step(mean, param, state):
        state_new = hold_rate * state + mean * rate
        return param - learn_rate * state_new, state_new

    def scattered(slope, dim):
        return lax.psum_scatter(slope[0].astype(BF16), "dp", scatter_dimension=dim, tiled=True).astype(F32)

    def gathered(value, dim):
        return lax.all_gather(value.astype(BF16), "dp", axis=dim, tiled=True)

    sums = lax.psum((slope_norm[0], slope_bias[0]), "dp")
    size = param_norm.shape[0]
    own = [lax.dynamic_slice_in_dim(v, place * size, size) for v in sums]
    nu, tu = step(scattered(slope_up, 0), param_up, state_up)
    nd, td = step(scattered(slope_down, 1), param_down, state_down)
    nn, tn = step(own[0], param_norm, state_norm)
    nb, tb = step(own[1], param_bias, state_bias)
    halves = gathered(nu, 0), gathered(nd, 1), gathered(nn, 0), gathered(nb, 0)
    return halves + (nu, nd, nn, nb, tu, td, tn, tb)


def body(*args):
    replicas = lax.axis_size("dp")
    chunk, columns = args[4].shape
    fits = replicas == 2 ** 3 and chunk % 16 == 0 and columns % (2 * LANES) == 0
    fits = fits and (replicas * chunk) % LANES == 0
    return (fused if fits else plain)(*args)


def solution(mesh):
    matrices = (P("dp", "tp"), P("tp", "dp"), P("dp"), P("dp"))
    return jax.shard_map(
        body,
        mesh=mesh,
        in_specs=(P("dp", None, "tp"), P("dp", "tp", None), P("dp", None), P("dp", None)) + matrices * 2,
        out_specs=(P(None, "tp"), P("tp", None), P(), P()) + matrices * 2,
        check_vma=False,
    )
```

```python
import functools
import math

import jax
import jax.numpy as jnp
from jax import lax
from jax.experimental import pallas as pl
from jax.experimental.pallas import tpu as pltpu
from jax.sharding import PartitionSpec as P

learn_rate = 0.1
hold_rate = 0.7
LANES = 128
GRANT_EXTRA = 2 * 1024 * 1024
F32 = jnp.float32
BF16 = jnp.bfloat16
FAR, NEAR, RS1, RS2, AG1, AG2, SH1, SH2, END, OVER = range(10)


def widths_of(half, small):
    if half < 2:
        return [half]
    if small:
        return [1] + widths_of(half - 1, False)
    return [half - half // 2, half // 2]


def slab_plan(columns):
    half = columns // LANES // 2
    slabs = []
    for m in (0, 1):
        start = 0
        for width in widths_of(half, m == 0):
            for axis in (0, 1):
                slabs.append((m, start, width * LANES, axis))
                start += width * LANES
    return slabs


def spot(k):
    y, x, core = k // 4, (k // 2) % 2, k % 2
    return (x, y, core) if core else (y, x, core)


def row_loop(rows, step, fn):
    def go(i, carry):
        fn(pl.ds(pl.multiple_of(i * step, step), step))
        return carry

    lax.fori_loop(0, rows // step, go, 0)


def kernel(
    replicas, slabs, order,
    su, sd, sn, sb, pu, pd, pn, pb, tu, td, tn, tb,
    gu, hd, par, sta, vg, vown,
    fu, fd, bu, bd, r0, r1, r2, gd, vin, vpar, vsta, vb, vr0, vr1, vr2,
    send_sem, recv_sem, vsend_sem, vrecv_sem, load_sem, par_sem, vec_sem,
):
    chunk, columns = pu.shape
    width = replicas * chunk
    me = lax.axis_index("dp")
    c = lax.rem(me, 2)
    x = lax.rem(me // 2, 2)
    y = me // 4
    mate = me + 1 - 2 * c
    x_peer, y_peer = me + 2 - 4 * x, me + 4 - 8 * y
    slow, fast = y + c * (x - y), x + c * (y - x)
    nbr = (x_peer + c * (y_peer - x_peer), y_peer + c * (x_peer - y_peer))
    rate = replicas ** (-0.5)
    step = 32 if chunk % 32 == 0 else 16
    count = len(slabs)
    per = len([s for s in slabs if s[0] == 0])
    b, g = (bu, bd), (gu, gd)
    V = count

    over = tuple(peer + 1 - 2 * c for peer in nbr)
    kept = chunk - chunk * 4 // 10 // 16 * 16

    barrier = pltpu.get_barrier_semaphore()
    for peer in (mate,) + nbr:
        pl.semaphore_signal(barrier, inc=1, device_id={"dp": peer}, device_id_type=pl.DeviceIdType.MESH)

    def local(src, dst, sem):
        cp = pltpu.make_async_copy(src, dst, sem)
        cp.start()
        return cp

    loads = {}
    for i, (m, lo, w, axis) in enumerate(slabs):
        if i > 3 and axis == 1:
            continue
        span = pl.ds(lo, w if i < 4 else 2 * w)
        if m == 0:
            loads[i] = local(su.at[0, :, span], fu.at[:, span], load_sem.at[len(loads)])
        else:
            loads[i] = local(sd.at[0, span], fd.at[span], load_sem.at[len(loads)])
    for n, (whole, pair) in enumerate(((vin, (sn, sb)), (vpar, (pn, pb)), (vsta, (tn, tb)))):
        for row in (0, 1):
            local(pair[row], whole.at[row], vec_sem.at[n])
    for n, (whole, pair) in enumerate(((par, (pu, pd)), (sta, (tu, td)))):
        for m in (0, 1):
            local(pair[m], whole.at[m], par_sem.at[n])

    def loaded(sem, *wholes):
        for n, whole in enumerate(wholes):
            pltpu.make_async_copy(whole, whole, sem.at[n]).wait()

    def convert(i):
        m, lo, w, _ = slabs[i]
        if i in loads:
            loads[i].wait()
        if m == 0:
            for k in range(replicas):
                bu[*spot(k), :, lo : lo + w] = fu[k * chunk : (k + 1) * chunk, lo : lo + w].astype(BF16)
        else:
            for block in range(width // LANES):
                first = block * LANES
                turned = fd[lo : lo + w, first : first + LANES].T.astype(BF16)
                done = 0
                while done < LANES:
                    k, off = divmod(first + done, chunk)
                    n = min(LANES - done, chunk - off)
                    bd[*spot(k), off : off + n, lo : lo + w] = turned[done : done + n]
                    done += n

    leave = {FAR: 0, NEAR: 0, AG2: 1, END: 1, SH1: 1, RS1: 2, SH2: 2, OVER: 2, RS2: 3, AG1: 3}
    vec_out = {FAR: 0, AG2: 0, SH1: 0, RS1: 1, SH2: 1, RS2: 2, AG1: 2}
    vec_in = {FAR: 0, AG1: 0, RS1: 1, AG2: 4, RS2: 2, SH1: 3, SH2: 3}

    half = count // 2

    def arrival(i, kind):
        if kind in (SH1, SH2, OVER):
            return 2 * count + (1 + (i - per) // 2 if slabs[i][0] else 0)
        if kind in (NEAR, END):
            return 2 * count + 1 + (count - per) // 2 + (kind == END)
        return i if kind in (FAR, AG1) else count + i // 2 + (half if kind == RS2 else 0)

    def remote(i, kind, src, dst, target):
        if i == V:
            sems = vsend_sem.at[vec_out[kind]], vrecv_sem.at[vec_in[kind]]
        else:
            sems = send_sem.at[leave[kind]], recv_sem.at[arrival(i, kind)]
        return pltpu.make_async_remote_copy(
            src_ref=src, dst_ref=dst, send_sem=sems[0], recv_sem=sems[1],
            device_id={"dp": target}, device_id_type=pl.DeviceIdType.MESH,
        )

    copies = {}

    def arrived(i, kind):
        m, lo, w, axis = slabs[i]
        if axis:
            return
        cols = pl.ds(lo, 2 * w)
        if kind == RS2:
            whole = r2.at[m, :, cols]
        else:
            whole = r1.at[m, :, pl.ds(0, kept if kind == AG2 and i < 2 else chunk), cols]
        remote(i, kind, whole, whole, mate).wait_recv()

    def copy(i, kind, src, dst, target):
        copies[i, kind] = remote(i, kind, src, dst, target)
        copies[i, kind].start()

    def sent(kind, whole):
        remote(0, kind, whole, whole, mate).wait_send()

    def swap(i, kind):
        m, lo, w, axis = slabs[i]
        cols = pl.ds(lo, w)
        if axis == 0:
            at = 1 - slow if kind == FAR else slow
            copy(i, kind, b[m].at[:, at, 1 - c, :, cols], r0.at[m, :, at, :, cols], mate)
        else:
            at = 1 - fast if kind == FAR else fast
            copy(i, kind, b[m].at[at, :, 1 - c, :, cols], r0.at[m, at, :, :, cols], mate)

    def rs1(i):
        m, lo, w, axis = slabs[i]
        cols = pl.ds(lo, w)
        copies[i, FAR].wait_recv()
        for j in (0, 1):
            at = (j, 1 - fast) if axis == 0 else (1 - slow, j)
            b[m][*at, c, :, lo : lo + w] = b[m][*at, c, :, lo : lo + w] + r0[m, *at, :, lo : lo + w]
        src = b[m].at[:, 1 - fast, c, :, cols] if axis == 0 else b[m].at[1 - slow, :, c, :, cols]
        copy(i, RS1, src, r1.at[m, :, :, cols], nbr[axis])

    def rs2(i):
        m, lo, w, axis = slabs[i]
        cs = slice(lo, lo + w)
        cols = pl.ds(lo, w)
        if i >= 4:
            arrived(i, RS1)
        j = 1 - slow if axis == 0 else 1 - fast
        far = (1 - slow, fast) if axis == 0 else (slow, 1 - fast)
        b[m][*far, c, :, cs] = b[m][*far, c, :, cs] + r0[m, *far, :, cs] + r1[m, j, :, cs]
        copy(i, RS2, b[m].at[*far, c, :, cols], r2.at[m, :, cols], nbr[1 - axis])
        own = slow, fast
        b[m][*own, c, :, cs] = b[m][*own, c, :, cs] + r0[m, *own, :, cs] + r1[m, 1 - j, :, cs]

    def update(i):
        m, lo, w, axis = slabs[i]
        cs = slice(lo, lo + w)
        cols = pl.ds(lo, w)
        arrived(i, RS2)
        own, out = b[m].at[slow, fast, c], g[m].at[slow, fast, c]

        def go(rows):
            mean = (own[rows, cs].astype(F32) + r2[m, rows, cs].astype(F32)) * rate
            state = hold_rate * sta[m, rows, cs] + mean
            new = par[m, rows, cs] - learn_rate * state
            out[rows, cs] = new.astype(BF16)
            sta[m, rows, cs] = state
            par[m, rows, cs] = new

        row_loop(chunk, step, go)
        copy(i, AG1, out.at[:, cols], out.at[:, cols], nbr[1 - axis])

    def ag2(i):
        m, lo, w, axis = slabs[i]
        cols = pl.ds(lo, w)
        copies[i, AG1].wait_recv()
        part = g[m].at[:, fast, c] if axis == 0 else g[m].at[slow, :, c]
        early = part.at[:, pl.ds(0, kept if i < 2 else chunk), cols]
        copy(i, AG2, early, early, nbr[axis])
        copy(i, SH1, part.at[:, :, cols], part.at[:, :, cols], mate)

    def ends():
        for i in (0, 1):
            m, lo, w, axis = slabs[i]
            part = g[m].at[:, fast, c] if axis == 0 else g[m].at[slow, :, c]
            rest = part.at[:, pl.ds(kept, chunk - kept), pl.ds(lo, w)]
            copy(i, END, rest, rest, nbr[axis])
            copy(i, OVER, rest, rest, over[axis])

    def share(i):
        m, lo, w, axis = slabs[i]
        cols = pl.ds(lo, w)
        arrived(i, AG2)
        part = g[m].at[:, 1 - fast, c] if axis == 0 else g[m].at[1 - slow, :, c]
        part = part.at[:, pl.ds(0, kept if i < 2 else chunk), cols]
        copy(i, SH2, part, part, mate)

    def finish(i):
        m, lo, w, axis = slabs[i]
        if m == 1:
            if axis == 0:
                pair = gd.at[:, :, 1 - c, :, pl.ds(lo, 2 * w)]
                remote(i, SH2, pair, pair, mate).wait_recv()
            for block in range(width // LANES):
                first, done, parts = block * LANES, 0, []
                while done < LANES:
                    k, off = divmod(first + done, chunk)
                    n = min(LANES - done, chunk - off)
                    parts.append(gd[*spot(k), off : off + n, lo : lo + w].astype(F32))
                    done += n
                whole = parts[0] if len(parts) == 1 else jnp.concatenate(parts, axis=0)
                hd[lo : lo + w, first : first + LANES] = whole.T.astype(BF16)

    def vec_swap():
        loaded(vec_sem, vin, vpar, vsta)
        for row in (0, 1):
            for k in range(replicas):
                vb[*spot(k), row : row + 1, 0:chunk] = vin[row, :, k * chunk : (k + 1) * chunk]
        copy(V, FAR, vb.at[:, :, 1 - c], vr0, mate)

    def vec_rs1():
        copies[V, FAR].wait_recv()
        for at in ((0, 0), (0, 1), (1, 0), (1, 1)):
            vb[*at, c] = vb[*at, c] + vr0[*at]
        copy(V, RS1, vb.at[:, 1 - fast, c], vr1, nbr[0])

    def vec_rs2():
        copies[V, RS1].wait_recv()
        for j in (0, 1):
            vb[j, fast, c] = vb[j, fast, c] + vr1[j]
        copy(V, RS2, vb.at[1 - slow, fast, c], vr2, nbr[1])

    def vec_update():
        copies[V, RS2].wait_recv()
        mean = (vb[slow, fast, c] + vr2[...]) * rate
        for row in (0, 1):
            state = hold_rate * vsta[row] + mean[row : row + 1, 0:chunk]
            new = vpar[row] - learn_rate * state
            vg[slow, fast, c, row : row + 1, 0:chunk] = new
            vown[row] = new
            vown[2 + row] = state
        copy(V, AG1, vg.at[slow, fast, c], vg.at[slow, fast, c], nbr[1])

    def vec_ag2():
        copies[V, AG1].wait_recv()
        part = vg.at[:, fast, c]
        copy(V, AG2, part, part, nbr[0])
        copy(V, SH1, part, part, mate)

    def vec_share():
        copies[V, AG2].wait_recv()
        part = vg.at[:, 1 - fast, c]
        copy(V, SH2, part, part, mate)

    vb[...] = jnp.zeros_like(vb)
    vg[slow, fast, c] = jnp.zeros(vr2.shape, F32)
    convert(0)
    pl.semaphore_wait(barrier, 3)
    swap(0, FAR)
    convert(1)
    swap(1, FAR)
    rs1(0)
    rs1(1)
    for i in range(2, count):
        if i == 4:
            rs1(2)
        convert(i)
        swap(i, FAR)
        if i > 4:
            rs1(i - 2)
        if i == 6:
            vec_swap()
        if i == 8:
            vec_rs1()
    for i in (count - 2, count - 1):
        rs1(i)
    for i in range(4):
        arrived(i, RS1)
    for i in range(count):
        swap(i, NEAR)
    remote(0, NEAR, r1, r1, mate).wait_recv()

    for i in range(count):
        rs2(i)
        if i == 4:
            sent(FAR, r0)
        if i == 7:
            vec_rs2()
    loaded(par_sem, par, sta)
    for n, i in enumerate(list(range(2, count)) + [0, 1]):
        update(i)
        if n == 6:
            vec_update()
    for n, i in enumerate(order):
        ag2(i)
        if n == 4:
            vec_ag2()
    ends()
    for n, i in enumerate(order):
        share(i)
        if n == 0:
            sent(RS2, r1)
        if n == 5:
            vec_share()
        if n == count - 2:
            other = vg.at[:, :, 1 - c]
            remote(V, SH2, other, other, mate).wait_recv()
            for whole, kind in ((vb, FAR), (vr0, RS1), (vr1, RS2)):
                remote(V, kind, whole, whole, mate).wait_send()
        if n > 1:
            finish(order[n - 2])
    finish(order[-2])
    finish(order[-1])
    rest = gu.at[:, 0, c, pl.ds(kept, chunk - kept), pl.ds(0, 2 * slabs[0][2])]
    remote(0, END, rest, rest, mate).wait_recv()
    whole = gu.at[:, :, 1 - c]
    remote(0, SH2, whole, whole, mate).wait_recv()
    sent(AG2, r0)
    sent(SH2, r0)


def spill(
    replicas, chunk,
    hu, hd, par, sta, vg, vown,
    hu_out, hd_out, nu_out, nd_out, tu_out, td_out, nn_out, nb_out, tn_out, tb_out, hn_out, hb_out,
    hv0, hv1, sem,
):
    width = replicas * chunk
    vw = columns_pad(chunk)
    for k in range(replicas):
        pltpu.make_async_copy(hu.at[*spot(k)], hu_out.at[pl.ds(k * chunk, chunk)], sem.at[0]).start()
    moves = [
        (hd, hd_out), (par.at[0], nu_out), (par.at[1], nd_out), (sta.at[0], tu_out), (sta.at[1], td_out),
        (vown.at[0], nn_out), (vown.at[1], nb_out), (vown.at[2], tn_out), (vown.at[3], tb_out),
        (hv0, hn_out), (hv1, hb_out),
    ]
    stores = [pltpu.make_async_copy(src, dst, sem.at[i + 1]) for i, (src, dst) in enumerate(moves)]
    for cp in stores[:-2]:
        cp.start()
    lane = lax.broadcasted_iota(jnp.int32, (2, width), 1)
    full = jnp.zeros((2, width), F32)
    for k in range(replicas):
        piece = vg[*spot(k)]
        wide = jnp.concatenate([piece, jnp.zeros((2, width - vw), F32)], axis=1) if width > vw else piece
        moved = pltpu.roll(wide, k * chunk, 1) if k else wide
        full = jnp.where((lane >= k * chunk) & (lane < (k + 1) * chunk), moved, full)
    for row, out in enumerate((hv0, hv1)):
        out[...] = full[row].astype(BF16)
    for cp in stores[-2:]:
        cp.start()
    for cp in stores:
        cp.wait()
    pltpu.make_async_copy(hu_out, hu_out, sem.at[0]).wait()


def columns_pad(n):
    return -(-n // LANES) * LANES


def fused(slope_up, slope_down, slope_norm, slope_bias, param_up, param_down, param_norm, param_bias,
          state_up, state_down, state_norm, state_bias):
    replicas = lax.axis_size("dp")
    chunk, columns = param_up.shape
    width = replicas * chunk
    slabs = slab_plan(columns)
    count = len(slabs)
    per = len([s for s in slabs if s[0] == 0])
    order = list(range(2, 4)) + list(range(per, count)) + list(range(4, per)) + [0, 1]
    vw = columns_pad(chunk)
    hbm = pl.BlockSpec(memory_space=pl.ANY)
    vmem = pl.BlockSpec(memory_space=pltpu.VMEM)
    cube = (2, 2, 2, chunk, columns)
    shape = jax.ShapeDtypeStruct
    dma = pltpu.SemaphoreType.DMA
    row = lambda v: v.reshape(1, -1)
    scratch = [
        pltpu.VMEM((width, columns), F32), pltpu.VMEM((columns, width), F32),
        pltpu.VMEM(cube, BF16), pltpu.VMEM(cube, BF16),
        pltpu.VMEM((2, 2, 2, chunk, columns), BF16),
        pltpu.VMEM((2, 2, chunk, columns), BF16),
        pltpu.VMEM((2, chunk, columns), BF16),
        pltpu.VMEM(cube, BF16),
        pltpu.VMEM((2, 1, width), F32), pltpu.VMEM((2, 1, chunk), F32), pltpu.VMEM((2, 1, chunk), F32),
        pltpu.VMEM((2, 2, 2, 2, vw), F32), pltpu.VMEM((2, 2, 2, vw), F32),
        pltpu.VMEM((2, 2, vw), F32), pltpu.VMEM((2, vw), F32),
    ]
    grant = sum(math.prod(s.shape) * jnp.dtype(s.dtype).itemsize for s in scratch) + GRANT_EXTRA
    hu, hd, par, sta, vg, vown = pl.pallas_call(
        functools.partial(kernel, replicas, slabs, order),
        out_shape=(
            pltpu.VMEM(cube, BF16), pltpu.VMEM((columns, width), BF16),
            pltpu.VMEM((2, chunk, columns), F32), pltpu.VMEM((2, chunk, columns), F32),
            pltpu.VMEM((2, 2, 2, 2, vw), F32), pltpu.VMEM((4, 1, chunk), F32),
        ),
        in_specs=[hbm] * 12,
        out_specs=[vmem] * 6,
        scratch_shapes=scratch + [
            dma((4,)), dma((2 * count + 3 + (count - per) // 2,)), dma((3,)), dma((5,)),
            dma((2 + count // 2,)), dma((2,)), dma((3,)),
        ],
        compiler_params=pltpu.CompilerParams(collective_id=0, has_side_effects=True, vmem_limit_bytes=grant),
    )(*(pltpu.with_memory_space_constraint(v, pltpu.HBM) for v in (
        slope_up, slope_down, slope_norm, slope_bias,
        param_up, param_down.T, row(param_norm), row(param_bias),
        state_up, state_down.T, row(state_norm), row(state_bias),
    )))
    block, line = shape((chunk, columns), F32), shape((1, chunk), F32)
    half = shape((width,), BF16)
    hu, hd, nu, nd, tu, td, nn, nb, tn, tb, hn, hb = pl.pallas_call(
        functools.partial(spill, replicas, chunk),
        out_shape=(shape((width, columns), BF16), shape((columns, width), BF16)) + (block,) * 4 + (line,) * 4 + (half,) * 2,
        in_specs=[vmem] * 6,
        out_specs=[hbm] * 12,
        scratch_shapes=[pltpu.VMEM((width,), BF16), pltpu.VMEM((width,), BF16), dma((12,))],
        compiler_params=pltpu.CompilerParams(vmem_limit_bytes=GRANT_EXTRA),
    )(hu, hd, par, sta, vg, vown)
    flat = lambda v: v.reshape(-1)
    return hu, hd, hn, hb, nu, nd.T, flat(nn), flat(nb), tu, td.T, flat(tn), flat(tb)


def plain(slope_up, slope_down, slope_norm, slope_bias, param_up, param_down, param_norm, param_bias,
          state_up, state_down, state_norm, state_bias):
    rate = lax.axis_size("dp") ** (-0.5)
    place = lax.axis_index("dp")

    def step(mean, param, state):
        state_new = hold_rate * state + mean * rate
        return param - learn_rate * state_new, state_new

    def scattered(slope, dim):
        return lax.psum_scatter(slope[0].astype(BF16), "dp", scatter_dimension=dim, tiled=True).astype(F32)

    def gathered(value, dim):
        return lax.all_gather(value.astype(BF16), "dp", axis=dim, tiled=True)

    sums = lax.psum((slope_norm[0], slope_bias[0]), "dp")
    size = param_norm.shape[0]
    own = [lax.dynamic_slice_in_dim(v, place * size, size) for v in sums]
    nu, tu = step(scattered(slope_up, 0), param_up, state_up)
    nd, td = step(scattered(slope_down, 1), param_down, state_down)
    nn, tn = step(own[0], param_norm, state_norm)
    nb, tb = step(own[1], param_bias, state_bias)
    halves = gathered(nu, 0), gathered(nd, 1), gathered(nn, 0), gathered(nb, 0)
    return halves + (nu, nd, nn, nb, tu, td, tn, tb)


def body(*args):
    replicas = lax.axis_size("dp")
    chunk, columns = args[4].shape
    fits = replicas == 2 ** 3 and chunk % 16 == 0 and columns % (2 * LANES) == 0
    fits = fits and (replicas * chunk) % LANES == 0
    return (fused if fits else plain)(*args)


def solution(mesh):
    matrices = (P("dp", "tp"), P("tp", "dp"), P("dp"), P("dp"))
    return jax.shard_map(
        body,
        mesh=mesh,
        in_specs=(P("dp", None, "tp"), P("dp", "tp", None), P("dp", None), P("dp", None)) + matrices * 2,
        out_specs=(P(None, "tp"), P("tp", None), P(), P()) + matrices * 2,
        check_vma=False,
    )
```
